128 devices in a mesh: obs: 4 (over y), cell: 32 (over z, x, core).
Axes of the slice: x: 4, y: 4, z: 4, core: 2. Of those that a mesh axis runs over, the one named last changes fastest.
Arguments:
- log_k: bfloat16 [6291456, 128], P(('obs', 'cell')), may hold values from -6 to 6
- heads_pred: bfloat16 [65536, 128], P(('obs', 'cell')), may hold values from -6 to 6
- slot_well: int32 [65536], P(('obs', 'cell')), may hold values from 0 to 16383, as said below
- tile_count: int32 [128], P(('obs', 'cell')), may hold values from 16 to 512, as said below
- obs_values: float32 [16384, 128], P(('obs', 'cell')), may hold values from -9 to 9
- obs_std: float32 [16384], P(('obs', 'cell')), may hold values from 0.5 to 2
- loc_blocks: int32 [32, 8], replicated, may hold values from 0 to 127, all different within a row
- taper: float32 [32, 8], replicated, may hold values from 0.3 to 1
- lambdas: float32 [4], replicated, may hold values from 0.1 to 10
Outputs:
- posterior: bfloat16 [6291456, 128], P(('obs', 'cell'))
- change_norms: float32 [128, 4, 128], P(('obs', 'cell'))
The draws below stay inside these ranges and needn't reach their ends.
Inputs may be any that keep to these rules, and one draw needn't show every extreme that they name: `slot_well`: slots below a cell block's count hold the wells lying in that block in increasing order; every well lies in exactly one cell block; other slots hold 0. No cell block holds more than 16 wells of one observation block, and some pairs hold exactly 16. `tile_count`: some cell blocks hold exactly 512 wells. `loc_blocks`: each row names 8 different blocks, and every block is named by some tile.
All inputs are finite; a program needn't handle non-finite values.
Results may differ from the reference program's by a relative error of at most 0.0095.
Values may be sent and summed in bfloat16 or wider, within the bound.
No kernel may reach another device: no remote copies, remote signals or barrier semaphores. Data moves between devices by JAX's collectives and lax.ppermute only.
A program may use at most 256 MiB of HBM per device.

```python
import math
import jax
import jax.numpy as jnp
from jax import lax

M = 128
CELL_DEV = 49152
W_DEV = 128
CAP = 16
LOC = 8
NLAM = 4
SLOTS = 512
HOT = 4
WELLS = 16384
CELLS = 6291456
N_CELL = 32
DEVICES = 128


def wells_layout(key):
    device_order = jax.random.permutation(jax.random.fold_in(key, 11), DEVICES)
    owner_keys = jax.random.split(jax.random.fold_in(key, 12), DEVICES)
    inner_order = jax.vmap(lambda k: jax.random.permutation(k, W_DEV))(owner_keys)
    pair_index = (inner_order.reshape(-1) // CAP).astype(jnp.int32)
    owner = jnp.arange(WELLS, dtype=jnp.int32) // W_DEV
    groups = W_DEV // CAP
    cold_total = DEVICES - HOT
    cold_index = (owner * (groups - 1) + pair_index - 1) % cold_total
    hot_source = device_order[owner % HOT]
    cold_source = device_order[HOT + cold_index]
    source = jnp.where(pair_index == 0, hot_source, cold_source).astype(jnp.int32)
    sort_score = source * WELLS + jnp.arange(WELLS, dtype=jnp.int32)
    ordering = jnp.argsort(sort_score).astype(jnp.int32)
    sorted_source = source[ordering]
    counts = jax.ops.segment_sum(jnp.ones((WELLS,), jnp.int32), source, DEVICES)
    starts = jnp.cumsum(counts) - counts
    slot_rank = jnp.arange(WELLS, dtype=jnp.int32) - starts[sorted_source]
    slot_table = jnp.zeros((DEVICES * SLOTS,), jnp.int32).at[sorted_source * SLOTS + slot_rank].set(ordering)
    return (slot_table, counts.astype(jnp.int32))


def draw_slot_well(key, part):
    return wells_layout(key)[0]


def draw_tile_count(key, part):
    return wells_layout(key)[1]


def block_scale(own_key, dims, cuts, least, high):
    level, own = 1.0, jax.random.fold_in(own_key, 6)
    for axis_at, blocks in cuts:
        heights = jnp.exp(jax.random.uniform(jax.random.fold_in(own, axis_at), (blocks,), jnp.float32, least / len(cuts), high / len(cuts)))
        level = level * jnp.repeat(heights, dims[axis_at] // blocks).reshape([-1 if axis == axis_at else 1 for axis in range(len(dims))])
    return level


def picks_of(own_key, rows, amount, top, lift):
    order = jax.random.permutation(jax.random.fold_in(own_key, 1), amount)
    pull = order
    for power in range(3):
        pull = pull * pull // amount
    pull = pull * lift // amount
    tickets = jax.random.randint(jax.random.fold_in(own_key, 2), (rows, amount), 0, 4096) + pull
    fixed_rows = jax.random.permutation(jax.random.fold_in(own_key, 3), rows)[jnp.arange(amount) % rows]
    tickets = jnp.where(jnp.arange(rows)[:, None] == fixed_rows[None, :], 1 << 14, tickets)
    score = tickets * amount + jnp.arange(amount)
    return lax.top_k(score.astype(jnp.int32), top)[1].astype(jnp.int32)


def noise(stream_key, dims, spread, reach, cuts=(), kind=jnp.bfloat16):
    drawn = spread * jax.random.normal(stream_key, dims, jnp.float32)
    if cuts:
        drawn = drawn * block_scale(stream_key, dims, cuts, -0.22, 0.18)
    return jnp.clip(drawn, -reach, reach).astype(kind)


def setup_inputs(seed: int = 0) -> dict:
    seeds = jax.random.split(jax.random.key(seed), 10)
    return {
        "log_k": noise(seeds[0], (CELLS, M), 1.0, 6.0, ((0, 128),)),
        "heads_pred": noise(seeds[1], (DEVICES * SLOTS, M), 1.0, 6.0, ((0, 128),)),
        "slot_well": draw_slot_well(jax.random.fold_in(seeds[9], 71), 0),
        "tile_count": draw_tile_count(jax.random.fold_in(seeds[9], 71), 0),
        "obs_values": noise(seeds[4], (WELLS, M), 1.5, 9.0, ((0, 128),), jnp.float32),
        "obs_std": jnp.clip(jnp.exp(math.log(2.0) - 1.3862944 * jax.random.uniform(seeds[5], (WELLS,), jnp.float32) ** block_scale(seeds[5], (WELLS,), ((0, 128),), -0.2, 0.2)), 0.5, 2.0),
        "loc_blocks": picks_of(seeds[6], N_CELL, DEVICES, LOC, 1024),
        "taper": jnp.clip(jax.random.uniform(seeds[7], (N_CELL, LOC), jnp.float32, 0.3, 1.0), 0.3, 1.0),
        "lambdas": jnp.clip(jnp.exp(jax.random.uniform(seeds[8], (NLAM,), jnp.float32, math.log(0.1), math.log(10.0))), 0.1, 10.0),
    }


def reference(log_k, heads_pred, slot_well, tile_count, obs_values, obs_std, loc_blocks, taper, lambdas):
    is_valid = jnp.arange(SLOTS, dtype=jnp.int32)[None, :] < tile_count[:, None]
    well_index = jnp.where(is_valid, slot_well.reshape(DEVICES, SLOTS), WELLS).reshape(-1).astype(jnp.int32)
    predicted = jnp.zeros((WELLS, M), jnp.float32).at[well_index].set(heads_pred.astype(jnp.float32), mode='drop')
    member_mean = jnp.mean(predicted, axis=1, keepdims=True)
    scaled = (predicted - member_mean) / obs_std[:, None]
    innovation = (obs_values - predicted) / obs_std[:, None]
    joined = jnp.concatenate([scaled, innovation], axis=1).reshape(DEVICES, W_DEV, 2 * M)
    scaled_blocks = scaled.reshape(DEVICES, W_DEV, M)
    block_gram = jnp.einsum('bwi,bwj->bij', scaled_blocks, joined, precision=lax.Precision.HIGHEST)
    matches = (loc_blocks[:, :, None] == jnp.arange(DEVICES, dtype=jnp.int32)[None, None, :]).astype(jnp.float32)
    tile_weights = jnp.sum(taper[:, :, None] * matches, axis=1)
    tile_gram = jnp.einsum('tb,bij->tij', tile_weights, block_gram, precision=lax.Precision.HIGHEST)
    curvature = tile_gram[:, :, :M]
    right_side = tile_gram[:, :, M:]
    identity = jnp.eye(M, dtype=jnp.float32)
    systems = curvature[:, None] + ((1.0 + lambdas) * (M - 1))[None, :, None, None] * identity
    transforms = jnp.linalg.solve(systems, jnp.broadcast_to(right_side[:, None], systems.shape))
    transforms = transforms.astype(jnp.bfloat16)
    joined_transforms = jnp.transpose(transforms, (0, 2, 1, 3)).reshape(N_CELL, M, NLAM * M)
    field_blocks = log_k.reshape(DEVICES, CELL_DEV, M)

    def update_block(inputs):
        block_field, block_index = inputs
        field = block_field.astype(jnp.float32)
        anomalies = (field - jnp.mean(field, axis=1, keepdims=True)).astype(jnp.bfloat16)
        tile_transform = joined_transforms[block_index % N_CELL]
        change = jnp.dot(anomalies.astype(jnp.float32), tile_transform.astype(jnp.float32), preferred_element_type=jnp.float32)
        change = change.reshape(CELL_DEV, NLAM, M)
        updated = (field + change[:, 0, :]).astype(jnp.bfloat16)
        return (updated, jnp.sum(change * change, axis=0))
    posterior, change_norms = lax.map(update_block, (field_blocks, jnp.arange(DEVICES, dtype=jnp.int32)))
    return (posterior.reshape(CELLS, M), change_norms)
```

```python
import jax
import jax.numpy as jnp
from jax import lax
from jax.experimental import pallas as pl
from jax.experimental.pallas import tpu as pltpu
from jax.sharding import PartitionSpec as P

CAP = 16
EXTRA = 8
F32 = jnp.float32
BF16 = jnp.bfloat16
HIGHEST = lax.Precision.HIGHEST
SMEM = pl.BlockSpec(memory_space=pltpu.SMEM)
VMEM = pl.BlockSpec(memory_space=pltpu.VMEM)
MIB = 1 << 20


def iota(shape, dim):
    return lax.broadcasted_iota(jnp.int32, shape, dim)


def one_hot(cond):
    return jnp.where(cond, 1.0, 0.0).astype(BF16)


def dot(a, b, contract=((1,), (0,)), precision=None):
    return lax.dot_general(
        a, b, (contract, ((), ())), precision=precision, preferred_element_type=F32
    )


def params(mib):
    return pltpu.CompilerParams(vmem_limit_bytes=mib * MIB)


def cost(flops, size):
    return pl.CostEstimate(flops=int(flops), bytes_accessed=int(size), transcendentals=0)


def send_rows(slot_well, tile_count, heads, n_obs, n_cell, wells_dev):
    slots, members = heads.shape
    rows = n_obs * CAP

    def body(count_ref, well_ref, heads_ref, out_ref):
        well = well_ref[...]
        valid = iota((1, slots), 1) < count_ref[0]
        block = jnp.where(valid, well // wells_dev, -1)
        place = well % wells_dev
        hits = one_hot(iota((n_obs * n_cell, slots), 0) == block)
        before = one_hot(iota((slots, slots), 0) < iota((slots, slots), 1))
        rank = jnp.sum(dot(hits, before) * hits.astype(F32), axis=0, keepdims=True)
        row = (block // n_cell) * CAP + rank.astype(jnp.int32)
        column = jnp.where(valid, block % n_cell, -1)
        target = jnp.where(valid, column * rows + row, -1)
        marks = jnp.where(iota((n_cell, slots), 0) == column, place + 1, 0)
        marks = marks.astype(F32).astype(BF16)
        places = dot(marks, one_hot(iota((members, slots), 0) == row), ((1,), (1,)))
        values = heads_ref[...]
        for c in range(n_cell):
            pick = one_hot(iota((rows, slots), 0) + c * rows == target)
            out_ref[c, 0:rows, :] = dot(pick, values).astype(BF16)
            out_ref[c, rows : rows + EXTRA, :] = jnp.broadcast_to(
                places[c : c + 1, :], (EXTRA, members)
            ).astype(BF16)

    return pl.pallas_call(
        body,
        out_shape=jax.ShapeDtypeStruct((n_cell, rows + EXTRA, members), BF16),
        in_specs=[SMEM, VMEM, VMEM],
        out_specs=VMEM,
        compiler_params=params(16),
        cost_estimate=cost(1e9, 1e6),
        name="send_rows",
    )(tile_count, slot_well.reshape(1, slots), heads)


def block_grams(place_obs, received, wells, n_obs):
    sources, height, members = received.shape
    rows = n_obs * CAP
    slots = sources * CAP
    wells_dev = wells[0].shape[0] - EXTRA
    band = members // n_obs

    def body(me_ref, recv_ref, *refs):
        well_refs, out_refs, gram_ref = refs[:n_obs], refs[n_obs : 2 * n_obs], refs[-1]
        me = me_ref[0]
        tail = recv_ref[:, rows : rows + EXTRA, :].astype(F32)
        places = jnp.max(tail, axis=1).astype(BF16)
        mine = iota((sources, slots), 0) == iota((sources, slots), 1) // CAP
        eye = iota((wells_dev, wells_dev), 0) == iota((wells_dev, wells_dev), 1)
        for k in range(n_obs):
            owner = lax.rem(me - k + n_obs, n_obs)
            first = owner * CAP
            spread = one_hot(
                iota((members, slots), 0) == iota((members, slots), 1) % CAP + first
            )
            spot = jnp.where(mine, dot(places, spread), 0.0)
            spot = jnp.sum(spot, axis=0, keepdims=True).astype(jnp.int32)
            pick = one_hot(iota((wells_dev, slots), 0) + 1 == spot)
            heads = recv_ref[:, pl.ds(pl.multiple_of(first, CAP), CAP), :]
            predicted = dot(pick, heads.reshape(slots, members))
            mean = jnp.sum(predicted, axis=1, keepdims=True) * (1.0 / members)
            deviation = well_refs[k][wells_dev : wells_dev + 1, :]
            deviation = jnp.sum(jnp.where(eye, deviation, 0.0), axis=1, keepdims=True)
            scale = 1.0 / deviation
            scaled = (predicted - mean) * scale
            innovation = (well_refs[k][0:wells_dev, :] - predicted) * scale
            joined = jnp.concatenate([scaled, innovation], axis=1)
            gram_ref[...] = dot(scaled.T, joined, precision=HIGHEST)
            for step in range(n_obs):
                dest = lax.rem(me + step, n_obs)
                part = gram_ref[pl.ds(pl.multiple_of(dest * band, band), band), :]
                out_refs[step][owner] = part.astype(BF16)

    return pl.pallas_call(
        body,
        out_shape=[jax.ShapeDtypeStruct((n_obs, band, 2 * members), BF16)] * n_obs,
        in_specs=[SMEM] + [VMEM] * (1 + n_obs),
        out_specs=[VMEM] * n_obs,
        scratch_shapes=[pltpu.VMEM((members, 2 * members), F32)],
        compiler_params=params(16),
        cost_estimate=cost(1e9, 1e6),
        name="block_grams",
    )(place_obs, received, *wells)


def tile_terms(weights, parts):
    n_tiles, n_obs = weights.shape
    _, band, width = parts[0].shape

    def body(weight_ref, *refs):
        out_ref = refs[-1]
        totals = []
        for o in range(n_obs):
            total = refs[0][o].astype(F32)
            for ref in refs[1:-1]:
                total = total + ref[o].astype(F32)
            totals.append(total)
        for t in range(n_tiles):
            term = weight_ref[t, 0] * totals[0]
            for o in range(1, n_obs):
                term = term + weight_ref[t, o] * totals[o]
            out_ref[t] = term.astype(BF16)

    return pl.pallas_call(
        body,
        out_shape=jax.ShapeDtypeStruct((n_tiles, band, width), BF16),
        in_specs=[SMEM] + [VMEM] * len(parts),
        out_specs=VMEM,
        compiler_params=params(16),
        cost_estimate=cost(1e8, 1e6),
        name="tile_terms",
    )(weights, *parts)


def invert_packed(packed, size, groups):
    lanes = size * groups
    lane = iota((size, lanes), 1)
    row = iota((size, lanes), 0)
    for j in range(size):
        column = jnp.take_along_axis(
            packed, lane // size * size + j, axis=1, mode="promise_in_bounds"
        )
        inverse = 1.0 / column[j : j + 1, :]
        pivot_row = packed[j : j + 1, :] * inverse
        here = lane % size == j
        others = jnp.where(here, -(column * inverse), packed - column * pivot_row)
        packed = jnp.where(row == j, jnp.where(here, inverse, pivot_row), others)
    return packed


def solve_all(place_obs, lambdas, bands, field_gram):
    n_obs = len(bands)
    band, width = bands[0].shape
    members = width // 2
    n_lam = lambdas.shape[0]
    size = members // n_lam

    def body(me_ref, lam_ref, *refs):
        band_refs = refs[:n_obs]
        gram_ref, out_ref, norm_ref, full_ref, work_ref = refs[n_obs:]
        me = me_ref[0]
        for k in range(n_obs):
            owner = lax.rem(me - k + n_obs, n_obs)
            full_ref[pl.ds(pl.multiple_of(owner * band, band), band), :] = band_refs[k][...]
        full = full_ref[...]
        diagonal = iota((members, width), 0) == iota((members, width), 1)
        for l in range(n_lam):
            shift = (1.0 + lam_ref[l]) * (members - 1)
            work_ref[l] = full + jnp.where(diagonal, shift, 0.0)
        lane = iota((size, members), 1)
        tall_lane = iota((members, members), 1)
        tall_row = iota((members, width), 0)
        for kb in range(members // size):
            at = kb * size
            packed = jnp.zeros((size, members), F32)
            for l in range(n_lam):
                piece = work_ref[l, at : at + size, 0:members]
                turn = (l - kb) * size % members
                piece = pltpu.roll(piece, turn, 1) if turn else piece
                packed = jnp.where(lane // size == l, piece, packed)
            packed = invert_packed(packed, size, n_lam)
            diag = jnp.concatenate(
                [jnp.where(lane // size == l, packed, 0.0) for l in range(n_lam)], axis=0
            )
            rows = jnp.concatenate(
                [work_ref[l, at : at + size, :] for l in range(n_lam)], axis=0
            )
            upper = dot(diag, rows, precision=HIGHEST)
            left = []
            for l in range(n_lam):
                piece = work_ref[l, :, 0:members]
                turn = (l - kb) * size % members
                piece = pltpu.roll(piece, turn, 1) if turn else piece
                left.append(jnp.where(tall_lane // size == l, piece, 0.0))
            delta = dot(jnp.concatenate(left, axis=0), upper, precision=HIGHEST)
            for l in range(n_lam):
                work_ref[l] = work_ref[l] - delta[l * members : (l + 1) * members, :]
                work_ref[l, at : at + size, :] = upper[l * size : (l + 1) * size, :]
        for l in range(n_lam):
            transform = work_ref[l, :, members:width].astype(BF16).astype(F32)
            spread = dot(gram_ref[...], transform, precision=HIGHEST)
            norm_ref[l : l + 1, :] = jnp.sum(transform * spread, axis=0, keepdims=True)
            if l == 0:
                mean = jnp.sum(transform, axis=0, keepdims=True) * (1.0 / members)
                centred = transform - mean
                high = centred.astype(BF16)
                out_ref[0:members, :] = high
                out_ref[members:width, :] = (centred - high.astype(F32)).astype(BF16)

    return pl.pallas_call(
        body,
        out_shape=[
            jax.ShapeDtypeStruct((width, members), BF16),
            jax.ShapeDtypeStruct((n_lam, members), F32),
        ],
        in_specs=[SMEM, SMEM] + [VMEM] * (n_obs + 1),
        out_specs=[VMEM, VMEM],
        scratch_shapes=[
            pltpu.VMEM((members, width), F32),
            pltpu.VMEM((n_lam, members, width), F32),
        ],
        compiler_params=params(16),
        cost_estimate=cost(1e9, 1e6),
        name="solve_all",
    )(place_obs, lambdas, *bands, field_gram)


def field_moments(log_k, start, count, chunk):
    members = log_k.shape[1]
    first = start // chunk

    def body(x_ref, out_ref):
        x = x_ref[...]
        spread = jnp.full((members, members), 1.0 / members, BF16)
        anomalies = (x.astype(F32) - dot(x, spread)).astype(BF16)
        part = dot(anomalies, anomalies, ((0,), (0,)))

        @pl.when(pl.program_id(0) == 0)
        def _():
            out_ref[...] = part

        @pl.when(pl.program_id(0) > 0)
        def _():
            out_ref[...] += part

    return pl.pallas_call(
        body,
        grid=(count // chunk,),
        out_shape=jax.ShapeDtypeStruct((members, members), F32),
        in_specs=[pl.BlockSpec((chunk, members), lambda i: (i + first, 0))],
        out_specs=pl.BlockSpec((members, members), lambda i: (0, 0)),
        compiler_params=params(16),
        cost_estimate=cost(6.0e9, count * members * 2),
        name="field_moments",
    )(log_k)


def update_field(log_k, transform, chunk):
    cells, members = log_k.shape

    def body(x_ref, t_ref, out_ref):
        x = x_ref[...]
        change = dot(jnp.concatenate([x, x], axis=1), t_ref[...])
        out_ref[...] = (x.astype(F32) + change).astype(BF16)

    return pl.pallas_call(
        body,
        grid=(cells // chunk,),
        out_shape=jax.ShapeDtypeStruct((cells, members), BF16),
        in_specs=[
            pl.BlockSpec((chunk, members), lambda i: (i, 0)),
            pl.BlockSpec((2 * members, members), lambda i: (0, 0)),
        ],
        out_specs=pl.BlockSpec((chunk, members), lambda i: (i, 0)),
        compiler_params=params(32),
        cost_estimate=cost(4 * cells * members * members, 4 * cells * members),
        name="update_field",
    )(log_k, transform)


def shifted(array, axis, step):
    n = lax.axis_size(axis)
    return lax.ppermute(array, axis, [(i, (i + step) % n) for i in range(n)])


def on_device(
    log_k, heads_pred, slot_well, tile_count, obs_values, obs_std, loc_blocks, taper, lambdas
):
    n_obs = lax.axis_size("obs")
    n_cell = lax.axis_size("cell")
    wells_dev, members = obs_values.shape
    place_obs = lax.axis_index("obs").astype(jnp.int32).reshape(1)
    sent = send_rows(slot_well, tile_count, heads_pred, n_obs, n_cell, wells_dev)
    received = lax.all_to_all(sent, "cell", split_axis=0, concat_axis=0, tiled=True)
    own_wells = jnp.concatenate(
        [obs_values, jnp.broadcast_to(obs_std[None], (EXTRA, wells_dev))], axis=0
    )
    wells = [own_wells] + [shifted(own_wells, "obs", k) for k in range(1, n_obs)]
    cells = log_k.shape[0]
    gram_a = field_moments(log_k, 0, cells // 2, 2048)
    gram_b = field_moments(log_k, cells // 2, cells // 2, 2048)
    column_blocks = jnp.arange(n_obs, dtype=jnp.int32) * n_cell + lax.axis_index("cell")
    weights = jnp.sum(
        taper[:, :, None]
        * (loc_blocks[:, :, None] == column_blocks[None, None, :]).astype(F32),
        axis=1,
    )
    grams = block_grams(place_obs, received, wells, n_obs)
    parts = [grams[0]] + [shifted(grams[k], "obs", k) for k in range(1, n_obs)]
    terms = tile_terms(weights, parts)
    gathered = lax.all_to_all(terms, "cell", split_axis=0, concat_axis=0, tiled=True)
    own_band = jnp.sum(gathered.astype(F32), axis=0)
    bands = [own_band] + [shifted(own_band, "obs", k) for k in range(1, n_obs)]
    transform, norms = solve_all(place_obs, lambdas, bands, gram_a + gram_b)
    return (update_field(log_k, transform, 4096), norms[None])


def solution(mesh):
    return jax.shard_map(
        on_device,
        mesh=mesh,
        in_specs=(
            P(("obs", "cell"), None),
            P(("obs", "cell"), None),
            P(("obs", "cell")),
            P(("obs", "cell")),
            P(("obs", "cell"), None),
            P(("obs", "cell")),
            P(),
            P(),
            P(),
        ),
        out_specs=(P(("obs", "cell"), None), P(("obs", "cell"), None, None)),
        check_vma=False,
    )
```

```python
import jax
import jax.numpy as jnp
from jax import lax
from jax.experimental import pallas as pl
from jax.experimental.pallas import tpu as pltpu
from jax.sharding import PartitionSpec as P


CAP = 16
EXTRA = 8
SPREAD = 16
F32 = jnp.float32
BF16 = jnp.bfloat16
HIGHEST = lax.Precision.HIGHEST
SMEM = pl.BlockSpec(memory_space=pltpu.SMEM)
VMEM = pl.BlockSpec(memory_space=pltpu.VMEM)
ANY = pl.BlockSpec(memory_space=pl.ANY)
MIB = 1 << 20


def iota(shape, dim):
    return lax.broadcasted_iota(jnp.int32, shape, dim)


def one_hot(cond):
    return jnp.where(cond, 1.0, 0.0).astype(BF16)


def dot(a, b, contract=((1,), (0,)), precision=None):
    return lax.dot_general(
        a, b, (contract, ((), ())), precision=precision, preferred_element_type=F32
    )


def params(mib):
    return pltpu.CompilerParams(vmem_limit_bytes=mib * MIB)


def cost(flops, size):
    return pl.CostEstimate(flops=int(flops), bytes_accessed=int(size), transcendentals=0)


def send_rows(slot_well, tile_count, heads, obs_values, obs_std, n_obs, n_cell):
    slots, members = heads.shape
    wells_dev = obs_values.shape[0]
    rows = n_obs * CAP

    def body(count_ref, well_ref, heads_ref, value_ref, std_ref, out_ref, join_ref):
        well = well_ref[...]
        valid = iota((1, slots), 1) < count_ref[0]
        block = jnp.where(valid, well // wells_dev, -1)
        place = well % wells_dev
        hits = one_hot(iota((n_obs * n_cell, slots), 0) == block)
        before = one_hot(iota((slots, slots), 0) < iota((slots, slots), 1))
        rank = jnp.sum(dot(hits, before) * hits.astype(F32), axis=0, keepdims=True)
        row = (block // n_cell) * CAP + rank.astype(jnp.int32)
        column = jnp.where(valid, block % n_cell, -1)
        target = jnp.where(valid, column * rows + row, -1)
        marks = jnp.where(iota((n_cell, slots), 0) == column, place + 1, 0)
        marks = marks.astype(F32).astype(BF16)
        places = dot(marks, one_hot(iota((members, slots), 0) == row), ((1,), (1,)))
        values = heads_ref[...]
        for c in range(n_cell):
            pick = one_hot(iota((rows, slots), 0) + c * rows == target)
            out_ref[c, 0:rows, :] = dot(pick, values).astype(BF16)
            out_ref[c, rows : rows + EXTRA, :] = jnp.broadcast_to(
                places[c : c + 1, :], (EXTRA, members)
            ).astype(BF16)
        join_ref[0:wells_dev, :] = value_ref[...]
        join_ref[wells_dev:, :] = jnp.broadcast_to(std_ref[...], (EXTRA, wells_dev))

    return pl.pallas_call(
        body,
        out_shape=[
            jax.ShapeDtypeStruct((n_cell, rows + EXTRA, members), BF16),
            jax.ShapeDtypeStruct((wells_dev + EXTRA, members), F32),
        ],
        in_specs=[SMEM] + [VMEM] * 4,
        out_specs=[VMEM, VMEM],
        compiler_params=params(60),
        cost_estimate=cost(1e9, 1e6),
        name="send_rows",
    )(tile_count, slot_well.reshape(1, slots), heads, obs_values, obs_std.reshape(1, wells_dev))


def block_grams(place_obs, received, wells, after, n_obs):
    sources, _, members = received.shape
    rows = n_obs * CAP
    slots = sources * CAP
    wells_dev = wells[0].shape[0] - EXTRA
    band = members // n_obs

    def body(me_ref, recv_ref, after_ref, *refs):
        well_refs, out_refs, gram_ref = refs[:n_obs], refs[n_obs : 2 * n_obs], refs[-1]
        me = me_ref[0]
        tail = recv_ref[:, rows : rows + EXTRA, :].astype(F32)
        places = jnp.max(tail, axis=1).astype(BF16)
        mine = iota((sources, slots), 0) == iota((sources, slots), 1) // CAP
        eye = iota((wells_dev, wells_dev), 0) == iota((wells_dev, wells_dev), 1)
        for k in range(n_obs):
            owner = lax.rem(me - k + n_obs, n_obs)
            first = owner * CAP
            spread = one_hot(
                iota((members, slots), 0) == iota((members, slots), 1) % CAP + first
            )
            spot = jnp.where(mine, dot(places, spread), 0.0)
            spot = jnp.sum(spot, axis=0, keepdims=True).astype(jnp.int32)
            pick = one_hot(iota((wells_dev, slots), 0) + 1 == spot)
            heads = recv_ref[:, pl.ds(pl.multiple_of(first, CAP), CAP), :]
            predicted = dot(pick, heads.reshape(slots, members))
            mean = jnp.sum(predicted, axis=1, keepdims=True) * (1.0 / members)
            deviation = well_refs[k][wells_dev : wells_dev + 1, :]
            deviation = jnp.sum(jnp.where(eye, deviation, 0.0), axis=1, keepdims=True)
            scale = 1.0 / deviation
            scaled = (predicted - mean) * scale
            offset = (well_refs[k][0:wells_dev, :] - mean) * scale
            joined = jnp.concatenate([scaled, offset], axis=1)
            gram_ref[...] = dot(scaled.T, joined, precision=HIGHEST)
            for step in range(n_obs):
                dest = lax.rem(me + step, n_obs)
                part = gram_ref[pl.ds(pl.multiple_of(dest * band, band), band), :]
                out_refs[step][owner] = part.astype(BF16)

    return pl.pallas_call(
        body,
        out_shape=[jax.ShapeDtypeStruct((n_obs, band, 2 * members), BF16)] * n_obs,
        in_specs=[SMEM] + [VMEM] * (2 + n_obs),
        out_specs=[VMEM] * n_obs,
        scratch_shapes=[pltpu.VMEM((members, 2 * members), F32)],
        compiler_params=params(16),
        cost_estimate=cost(1e9, 1e6),
        name="block_grams",
    )(place_obs, received, after, *wells)


def tile_terms(weights, parts):
    n_tiles, n_obs = weights.shape
    _, band, width = parts[0].shape

    def body(weight_ref, *refs):
        out_ref = refs[-1]
        totals = []
        for o in range(n_obs):
            total = refs[0][o].astype(F32)
            for ref in refs[1:-1]:
                total = total + ref[o].astype(F32)
            totals.append(total)
        for t in range(n_tiles):
            term = weight_ref[t, 0] * totals[0]
            for o in range(1, n_obs):
                term = term + weight_ref[t, o] * totals[o]
            out_ref[t] = term.astype(BF16)

    return pl.pallas_call(
        body,
        out_shape=jax.ShapeDtypeStruct((n_tiles, band, width), BF16),
        in_specs=[SMEM] + [VMEM] * len(parts),
        out_specs=VMEM,
        compiler_params=params(16),
        cost_estimate=cost(1e8, 1e6),
        name="tile_terms",
    )(weights, *parts)


def invert_packed(packed, size, groups):
    lanes = size * groups
    lane = iota((size, lanes), 1)
    row = iota((size, lanes), 0)
    for j in range(size):
        column = jnp.take_along_axis(
            packed, lane // size * size + j, axis=1, mode="promise_in_bounds"
        )
        inverse = 1.0 / column[j : j + 1, :]
        pivot_row = packed[j : j + 1, :] * inverse
        here = lane % size == j
        others = jnp.where(here, -(column * inverse), packed - column * pivot_row)
        packed = jnp.where(row == j, jnp.where(here, inverse, pivot_row), others)
    return packed


def halves(a):
    high = a.astype(BF16)
    return high, (a - high.astype(F32)).astype(BF16)


def finish(place_obs, lambdas, bands, field_gram, log_k, count):
    n_obs = len(bands)
    band, width = bands[0].shape
    members = width // 2
    n_lam = lambdas.shape[0]
    size = members // n_lam
    cells = log_k.shape[0]
    chunk = cells // count

    def eliminate(lam_ref, full_ref, work_ref, answer_ref):
        eye = iota((members, members), 0) == iota((members, members), 1)
        for l in range(n_lam):
            shift = (1.0 + lam_ref[l]) * (members - 1)
            system = full_ref[:, 0:members] + jnp.where(eye, shift, 0.0)
            known = dot(system, answer_ref[l], precision=HIGHEST)
            work_ref[l, :, 0:members] = system
            work_ref[l, :, members:width] = full_ref[:, members:width] - known
        lane = iota((size, members), 1)
        tall_lane = iota((members, members), 1)
        for kb in range(members // size):
            at = kb * size
            packed = jnp.zeros((size, members), F32)
            for l in range(n_lam):
                piece = work_ref[l, at : at + size, 0:members]
                turn = (l - kb) * size % members
                piece = pltpu.roll(piece, turn, 1) if turn else piece
                packed = jnp.where(lane // size == l, piece, packed)
            packed = invert_packed(packed, size, n_lam)
            diag = jnp.concatenate(
                [jnp.where(lane // size == l, packed, 0.0) for l in range(n_lam)], axis=0
            )
            rows = jnp.concatenate(
                [work_ref[l, at : at + size, :] for l in range(n_lam)], axis=0
            )
            upper = dot(diag, rows, precision=HIGHEST)
            left = []
            for l in range(n_lam):
                piece = work_ref[l, :, 0:members]
                turn = (l - kb) * size % members
                piece = pltpu.roll(piece, turn, 1) if turn else piece
                left.append(jnp.where(tall_lane // size == l, piece, 0.0))
            delta = dot(jnp.concatenate(left, axis=0), upper, precision=HIGHEST)
            for l in range(n_lam):
                work_ref[l] = work_ref[l] - delta[l * members : (l + 1) * members, :]
                work_ref[l, at : at + size, :] = upper[l * size : (l + 1) * size, :]
        for l in range(n_lam):
            answer_ref[l] = answer_ref[l] + work_ref[l, :, members:width]

    def body(me_ref, lam_ref, *refs):
        band_refs = refs[:n_obs]
        gram_ref, field_ref, out_ref, norm_ref = refs[n_obs : n_obs + 4]
        full_ref, work_ref, power_ref, inverse_ref, answer_ref = refs[n_obs + 4 : n_obs + 9]
        hold_ref, in_sem, out_sem = refs[n_obs + 9 :]
        loads, stores = [], []
        for i in range(count):
            rows = pl.ds(i * chunk, chunk)
            loads.append(pltpu.make_async_copy(field_ref.at[rows], hold_ref.at[i], in_sem.at[i]))
            stores.append(pltpu.make_async_copy(hold_ref.at[i], out_ref.at[rows], out_sem.at[i]))
            loads[i].start()
        me = me_ref[0]
        for k in range(n_obs):
            owner = lax.rem(me - k + n_obs, n_obs)
            full_ref[pl.ds(pl.multiple_of(owner * band, band), band), :] = band_refs[k][...]
        curvature = full_ref[:, 0:members]
        right = full_ref[:, members:width] - curvature
        share = 1.0 / members
        right = right - jnp.sum(right, axis=0, keepdims=True) * share
        curvature = curvature - jnp.sum(curvature, axis=0, keepdims=True) * share
        curvature = curvature - jnp.sum(curvature, axis=1, keepdims=True) * share
        full_ref[:, 0:members] = curvature
        full_ref[:, members:width] = right
        eye = iota((members, members), 0) == iota((members, members), 1)
        bound = jnp.max(jnp.sum(jnp.abs(curvature), axis=0, keepdims=True))
        shifts = [(1.0 + lam_ref[l]) * (members - 1) for l in range(n_lam)]
        least = shifts[0]
        for shift in shifts[1:]:
            least = jnp.minimum(least, shift)
        rate = bound / (bound + 2.0 * least)
        for l in range(n_lam):
            alpha = 2.0 / (bound + 2.0 * shifts[l])
            rest = jnp.where(eye, 1.0 - alpha * shifts[l], 0.0) - alpha * curvature
            inverse_ref[l] = alpha * (jnp.where(eye, 1.0, 0.0) + rest)
            rest = rest.astype(BF16)
            power_ref[l] = dot(rest, rest).astype(BF16)

        def going(state):
            return jnp.logical_and(state[0] > 0.02, state[1] < 24)

        def squared(state):
            for l in range(n_lam):
                power = power_ref[l]
                both = jnp.concatenate([power, inverse_ref[l].astype(BF16)], axis=1)
                step = dot(power, both)
                inverse_ref[l] = inverse_ref[l] + step[:, members:width]
                power_ref[l] = step[:, 0:members].astype(BF16)
            return state[0] * state[0], state[1] + 1

        lax.while_loop(going, squared, (rate * rate, jnp.int32(0)))
        inverses = [inverse_ref[l].astype(BF16) for l in range(n_lam)]
        right_low = right.astype(BF16)
        answers = [dot(inverse, right_low) for inverse in inverses]
        high, low = halves(curvature)
        wide = jnp.concatenate([high, low], axis=1)
        sizes = []
        for _ in range(2):
            changes = []
            for l in range(0, n_lam, 2):
                pair = jnp.concatenate(answers[l : l + 2], axis=1)
                top, bottom = halves(pair)
                product = dot(wide, jnp.concatenate([top, top], axis=0)) + dot(high, bottom)
                for q in range(2):
                    part = product[:, q * members : (q + 1) * members]
                    left = right - (part + shifts[l + q] * answers[l + q])
                    changes.append(dot(inverses[l + q], left.astype(BF16)))
            answers = [a + c for a, c in zip(answers, changes)]
            sizes.append([jnp.max(jnp.abs(c), axis=0, keepdims=True) for c in changes])
        good = None
        for l in range(n_lam):
            whole = jnp.max(jnp.max(jnp.abs(answers[l]), axis=0, keepdims=True))
            first, second = jnp.max(sizes[0][l]), jnp.max(sizes[1][l])
            fine = jnp.logical_and(second <= 1e-3 * whole, second <= jnp.maximum(0.2 * first, 1e-5 * whole))
            good = fine if good is None else jnp.logical_and(good, fine)
            answer_ref[l] = answers[l]

        @pl.when(jnp.logical_not(good))
        def _():
            answer_ref[...] = jnp.zeros_like(answer_ref)

            def improve(i, carry):
                eliminate(lam_ref, full_ref, work_ref, answer_ref)
                return carry

            lax.fori_loop(0, 2, improve, 0)

        transform = answer_ref[0].astype(BF16).astype(F32)
        step = (iota((members, members), 0) - iota((members, members), 1)) % members
        for start in (1, 1 + SPREAD):
            excess = jnp.sum(transform, axis=0, keepdims=True) * (1.0 / SPREAD)
            chosen = jnp.logical_and(step >= start, step < start + SPREAD)
            moved = jnp.where(chosen, transform - excess, transform)
            transform = moved.astype(BF16).astype(F32)
        transform = transform.astype(BF16)
        for i in range(count):
            loads[i].wait()
            x = hold_ref[i]
            hold_ref[i] = (x.astype(F32) + dot(x, transform)).astype(BF16)
            stores[i].start()
        moments = gram_ref[...]
        top, low = halves(moments)
        rest = moments - top.astype(F32)
        middle, low = halves(rest)
        wide = jnp.concatenate([top, middle], axis=1)
        for l in range(0, n_lam, 2):
            pair = jnp.concatenate([answer_ref[l], answer_ref[l + 1]], axis=1).astype(BF16)
            spread = dot(wide, jnp.concatenate([pair, pair], axis=0)) + dot(low, pair)
            totals = jnp.sum(pair.astype(F32) * spread, axis=0, keepdims=True)
            for q in range(2):
                norm_ref[l + q : l + q + 1, :] = totals[:, q * members : (q + 1) * members]
        for store in stores:
            store.wait()

    return pl.pallas_call(
        body,
        out_shape=[
            jax.ShapeDtypeStruct((cells, members), BF16),
            jax.ShapeDtypeStruct((n_lam, members), F32),
        ],
        in_specs=[SMEM, SMEM] + [VMEM] * (n_obs + 1) + [ANY],
        out_specs=[ANY, VMEM],
        scratch_shapes=[
            pltpu.VMEM((members, width), F32),
            pltpu.VMEM((n_lam, members, width), F32),
            pltpu.VMEM((n_lam, members, members), BF16),
            pltpu.VMEM((n_lam, members, members), F32),
            pltpu.VMEM((n_lam, members, members), F32),
            pltpu.VMEM((count, chunk, members), BF16),
            pltpu.SemaphoreType.DMA((count,)),
            pltpu.SemaphoreType.DMA((count,)),
        ],
        compiler_params=params(52),
        cost_estimate=cost(2e9, 4 * cells * members),
        name="finish",
    )(place_obs, lambdas, *bands, field_gram, log_k)


def field_moments(log_k, total, first, chunk, count):
    members = log_k.shape[1]

    def body(x_ref, total_ref, out_ref, hold_ref, sem):
        copies = []
        for i in range(count):
            rows = pl.ds(first + i * chunk, chunk)
            copies.append(pltpu.make_async_copy(x_ref.at[rows], hold_ref.at[i], sem.at[i]))
            copies[i].start()
        spread = jnp.full((members, members), 1.0 / members, BF16)
        moments = total_ref[...]
        for i in range(count):
            copies[i].wait()
            x = hold_ref[i]
            anomalies = (x.astype(F32) - dot(x, spread)).astype(BF16)
            moments = moments + dot(anomalies, anomalies, ((0,), (0,)))
        out_ref[...] = moments

    return pl.pallas_call(
        body,
        out_shape=jax.ShapeDtypeStruct((members, members), F32),
        in_specs=[ANY, VMEM],
        out_specs=VMEM,
        scratch_shapes=[
            pltpu.VMEM((count, chunk, members), BF16),
            pltpu.SemaphoreType.DMA((count,)),
        ],
        compiler_params=params(52),
        cost_estimate=cost(6.0e9, count * chunk * members * 2),
        name="field_moments",
    )(log_k, total)


def sum_band(gathered, after):
    n_tiles, band, width = gathered.shape

    def body(gathered_ref, after_ref, out_ref):
        total = gathered_ref[0].astype(F32)
        for t in range(1, n_tiles):
            total = total + gathered_ref[t].astype(F32)
        out_ref[...] = total

    return pl.pallas_call(
        body,
        out_shape=jax.ShapeDtypeStruct((band, width), F32),
        in_specs=[VMEM, VMEM],
        out_specs=VMEM,
        compiler_params=params(8),
        cost_estimate=cost(1e7, 1e6),
        name="sum_band",
    )(gathered, after)


def shifted(array, axis, step):
    n = lax.axis_size(axis)
    return lax.ppermute(array, axis, [(i, (i + step) % n) for i in range(n)])


def on_device(
    log_k, heads_pred, slot_well, tile_count, obs_values, obs_std, loc_blocks, taper, lambdas
):
    n_obs = lax.axis_size("obs")
    n_cell = lax.axis_size("cell")
    members = heads_pred.shape[1]
    place_obs = lax.axis_index("obs").astype(jnp.int32).reshape(1)
    sent, own_wells = send_rows(
        slot_well, tile_count, heads_pred, obs_values, obs_std, n_obs, n_cell
    )
    received = lax.all_to_all(sent, "cell", split_axis=0, concat_axis=0, tiled=True)
    wells = [own_wells] + [shifted(own_wells, "obs", k) for k in range(1, n_obs)]
    cells = log_k.shape[0]
    chunk = cells // 6
    moments = jnp.zeros((members, members), F32)
    moments = field_moments(log_k, moments, 0, chunk, 3)
    column_blocks = jnp.arange(n_obs, dtype=jnp.int32) * n_cell + lax.axis_index("cell")
    weights = jnp.sum(
        taper[:, :, None]
        * (loc_blocks[:, :, None] == column_blocks[None, None, :]).astype(F32),
        axis=1,
    )
    grams = block_grams(place_obs, received, wells, moments, n_obs)
    parts = [grams[0]] + [shifted(grams[k], "obs", k) for k in range(1, n_obs)]
    terms = tile_terms(weights, parts)
    gathered = lax.all_to_all(terms, "cell", split_axis=0, concat_axis=0, tiled=True)
    moments = field_moments(log_k, moments, 3 * chunk, chunk, 3)
    own_band = sum_band(gathered, moments)
    bands = [own_band] + [shifted(own_band, "obs", k) for k in range(1, n_obs)]
    posterior, norms = finish(place_obs, lambdas, bands, moments, log_k, 6)
    return (posterior, norms[None])


def solution(mesh):
    return jax.shard_map(
        on_device,
        mesh=mesh,
        in_specs=(
            P(("obs", "cell"), None),
            P(("obs", "cell"), None),
            P(("obs", "cell")),
            P(("obs", "cell")),
            P(("obs", "cell"), None),
            P(("obs", "cell")),
            P(),
            P(),
            P(),
        ),
        out_specs=(P(("obs", "cell"), None), P(("obs", "cell"), None, None)),
        check_vma=False,
    )
```

```python
import jax
import jax.numpy as jnp
from jax import lax
from jax.experimental import pallas as pl
from jax.experimental.pallas import tpu as pltpu
from jax.sharding import PartitionSpec as P


CAP = 16
EXTRA = 8
SPREAD = 16
TILE = 512
F32 = jnp.float32
BF16 = jnp.bfloat16
HIGHEST = lax.Precision.HIGHEST
SMEM = pl.BlockSpec(memory_space=pltpu.SMEM)
VMEM = pl.BlockSpec(memory_space=pltpu.VMEM)
ANY = pl.BlockSpec(memory_space=pl.ANY)
MIB = 1 << 20


def iota(shape, dim):
    return lax.broadcasted_iota(jnp.int32, shape, dim)


def one_hot(cond):
    return jnp.where(cond, 1.0, 0.0).astype(BF16)


def dot(a, b, contract=((1,), (0,)), precision=None):
    return lax.dot_general(
        a, b, (contract, ((), ())), precision=precision, preferred_element_type=F32
    )


def params(mib):
    return pltpu.CompilerParams(vmem_limit_bytes=mib * MIB)


def cost(flops, size):
    return pl.CostEstimate(flops=int(flops), bytes_accessed=int(size), transcendentals=0)


def send_rows(slot_well, tile_count, heads, obs_values, obs_std, n_obs, n_cell):
    slots, members = heads.shape
    wells_dev = obs_values.shape[0]
    rows = n_obs * CAP

    def body(count_ref, well_ref, heads_ref, value_ref, std_ref, out_ref, join_ref):
        well = well_ref[...]
        valid = iota((1, slots), 1) < count_ref[0]
        block = jnp.where(valid, well // wells_dev, -1)
        place = well % wells_dev
        hits = one_hot(iota((n_obs * n_cell, slots), 0) == block)
        before = one_hot(iota((slots, slots), 0) < iota((slots, slots), 1))
        rank = jnp.sum(dot(hits, before) * hits.astype(F32), axis=0, keepdims=True)
        row = (block // n_cell) * CAP + rank.astype(jnp.int32)
        column = jnp.where(valid, block % n_cell, -1)
        target = jnp.where(valid, column * rows + row, -1)
        marks = jnp.where(iota((n_cell, slots), 0) == column, place + 1, 0)
        marks = marks.astype(F32).astype(BF16)
        places = dot(marks, one_hot(iota((members, slots), 0) == row), ((1,), (1,)))
        values = heads_ref[...]
        for c in range(n_cell):
            pick = one_hot(iota((rows, slots), 0) + c * rows == target)
            out_ref[c, 0:rows, :] = dot(pick, values).astype(BF16)
            out_ref[c, rows : rows + EXTRA, :] = jnp.broadcast_to(
                places[c : c + 1, :], (EXTRA, members)
            ).astype(BF16)
        join_ref[0:wells_dev, :] = value_ref[...]
        join_ref[wells_dev:, :] = jnp.broadcast_to(std_ref[...], (EXTRA, wells_dev))

    return pl.pallas_call(
        body,
        out_shape=[
            jax.ShapeDtypeStruct((n_cell, rows + EXTRA, members), BF16),
            jax.ShapeDtypeStruct((wells_dev + EXTRA, members), F32),
        ],
        in_specs=[SMEM] + [VMEM] * 4,
        out_specs=[VMEM, VMEM],
        compiler_params=params(60),
        cost_estimate=cost(1e9, 1e6),
        name="send_rows",
    )(tile_count, slot_well.reshape(1, slots), heads, obs_values, obs_std.reshape(1, wells_dev))


def block_grams(place_obs, received, wells, after, n_obs):
    sources, _, members = received.shape
    rows = n_obs * CAP
    slots = sources * CAP
    wells_dev = wells[0].shape[0] - EXTRA
    band = members // n_obs

    def body(me_ref, recv_ref, after_ref, *refs):
        well_refs, out_refs, gram_ref = refs[:n_obs], refs[n_obs : 2 * n_obs], refs[-1]
        me = me_ref[0]
        tail = recv_ref[:, rows : rows + EXTRA, :].astype(F32)
        places = jnp.max(tail, axis=1).astype(BF16)
        mine = iota((sources, slots), 0) == iota((sources, slots), 1) // CAP
        eye = iota((wells_dev, wells_dev), 0) == iota((wells_dev, wells_dev), 1)
        for k in range(n_obs):
            owner = lax.rem(me - k + n_obs, n_obs)
            first = owner * CAP
            spread = one_hot(
                iota((members, slots), 0) == iota((members, slots), 1) % CAP + first
            )
            spot = jnp.where(mine, dot(places, spread), 0.0)
            spot = jnp.sum(spot, axis=0, keepdims=True).astype(jnp.int32)
            pick = one_hot(iota((wells_dev, slots), 0) + 1 == spot)
            heads = recv_ref[:, pl.ds(pl.multiple_of(first, CAP), CAP), :]
            predicted = dot(pick, heads.reshape(slots, members))
            mean = jnp.sum(predicted, axis=1, keepdims=True) * (1.0 / members)
            deviation = well_refs[k][wells_dev : wells_dev + 1, :]
            deviation = jnp.sum(jnp.where(eye, deviation, 0.0), axis=1, keepdims=True)
            scale = 1.0 / deviation
            scaled = (predicted - mean) * scale
            offset = (well_refs[k][0:wells_dev, :] - mean) * scale
            joined = jnp.concatenate([scaled, offset], axis=1)
            gram_ref[...] = dot(scaled.T, joined, precision=HIGHEST)
            for step in range(n_obs):
                dest = lax.rem(me + step, n_obs)
                part = gram_ref[pl.ds(pl.multiple_of(dest * band, band), band), :]
                out_refs[step][owner] = part.astype(BF16)

    return pl.pallas_call(
        body,
        out_shape=[jax.ShapeDtypeStruct((n_obs, band, 2 * members), BF16)] * n_obs,
        in_specs=[SMEM] + [VMEM] * (2 + n_obs),
        out_specs=[VMEM] * n_obs,
        scratch_shapes=[pltpu.VMEM((members, 2 * members), F32)],
        compiler_params=params(16),
        cost_estimate=cost(1e9, 1e6),
        name="block_grams",
    )(place_obs, received, after, *wells)


def tile_terms(weights, parts):
    n_tiles, n_obs = weights.shape
    _, band, width = parts[0].shape

    def body(weight_ref, *refs):
        out_ref = refs[-1]
        totals = []
        for o in range(n_obs):
            total = refs[0][o].astype(F32)
            for ref in refs[1:-1]:
                total = total + ref[o].astype(F32)
            totals.append(total)
        for t in range(n_tiles):
            term = weight_ref[t, 0] * totals[0]
            for o in range(1, n_obs):
                term = term + weight_ref[t, o] * totals[o]
            out_ref[t] = term.astype(BF16)

    return pl.pallas_call(
        body,
        out_shape=jax.ShapeDtypeStruct((n_tiles, band, width), BF16),
        in_specs=[SMEM] + [VMEM] * len(parts),
        out_specs=VMEM,
        compiler_params=params(16),
        cost_estimate=cost(1e8, 1e6),
        name="tile_terms",
    )(weights, *parts)


def invert_packed(packed, size, groups):
    lanes = size * groups
    lane = iota((size, lanes), 1)
    row = iota((size, lanes), 0)
    for j in range(size):
        column = jnp.take_along_axis(
            packed, lane // size * size + j, axis=1, mode="promise_in_bounds"
        )
        inverse = 1.0 / column[j : j + 1, :]
        pivot_row = packed[j : j + 1, :] * inverse
        here = lane % size == j
        others = jnp.where(here, -(column * inverse), packed - column * pivot_row)
        packed = jnp.where(row == j, jnp.where(here, inverse, pivot_row), others)
    return packed


def halves(a):
    high = a.astype(BF16)
    return high, (a - high.astype(F32)).astype(BF16)


def finish(place_obs, lambdas, bands, field_gram, log_k, count):
    n_obs = len(bands)
    band, width = bands[0].shape
    members = width // 2
    n_lam = lambdas.shape[0]
    size = members // n_lam
    cells = log_k.shape[0]
    chunk = cells // count

    def eliminate(lam_ref, full_ref, work_ref, answer_ref):
        eye = iota((members, members), 0) == iota((members, members), 1)
        for l in range(n_lam):
            shift = (1.0 + lam_ref[l]) * (members - 1)
            system = full_ref[:, 0:members] + jnp.where(eye, shift, 0.0)
            known = dot(system, answer_ref[l], precision=HIGHEST)
            work_ref[l, :, 0:members] = system
            work_ref[l, :, members:width] = full_ref[:, members:width] - known
        lane = iota((size, members), 1)
        tall_lane = iota((members, members), 1)
        for kb in range(members // size):
            at = kb * size
            packed = jnp.zeros((size, members), F32)
            for l in range(n_lam):
                piece = work_ref[l, at : at + size, 0:members]
                turn = (l - kb) * size % members
                piece = pltpu.roll(piece, turn, 1) if turn else piece
                packed = jnp.where(lane // size == l, piece, packed)
            packed = invert_packed(packed, size, n_lam)
            diag = jnp.concatenate(
                [jnp.where(lane // size == l, packed, 0.0) for l in range(n_lam)], axis=0
            )
            rows = jnp.concatenate(
                [work_ref[l, at : at + size, :] for l in range(n_lam)], axis=0
            )
            upper = dot(diag, rows, precision=HIGHEST)
            left = []
            for l in range(n_lam):
                piece = work_ref[l, :, 0:members]
                turn = (l - kb) * size % members
                piece = pltpu.roll(piece, turn, 1) if turn else piece
                left.append(jnp.where(tall_lane // size == l, piece, 0.0))
            delta = dot(jnp.concatenate(left, axis=0), upper, precision=HIGHEST)
            for l in range(n_lam):
                work_ref[l] = work_ref[l] - delta[l * members : (l + 1) * members, :]
                work_ref[l, at : at + size, :] = upper[l * size : (l + 1) * size, :]
        for l in range(n_lam):
            answer_ref[l] = answer_ref[l] + work_ref[l, :, members:width]

    def body(me_ref, lam_ref, *refs):
        band_refs = refs[:n_obs]
        gram_ref, field_ref, out_ref, norm_ref = refs[n_obs : n_obs + 4]
        full_ref, work_ref, power_ref, inverse_ref, answer_ref = refs[n_obs + 4 : n_obs + 9]
        hold_ref, made_ref, in_sem, out_sem = refs[n_obs + 9 :]
        loads, stores = [], []
        for i in range(count):
            rows = pl.ds(i * chunk, chunk)
            loads.append(pltpu.make_async_copy(field_ref.at[rows], hold_ref.at[i], in_sem.at[i]))
            stores.append(pltpu.make_async_copy(made_ref.at[i], out_ref.at[rows], out_sem.at[i]))
            loads[i].start()
        me = me_ref[0]
        for k in range(n_obs):
            owner = lax.rem(me - k + n_obs, n_obs)
            full_ref[pl.ds(pl.multiple_of(owner * band, band), band), :] = band_refs[k][...]
        curvature = full_ref[:, 0:members]
        right = full_ref[:, members:width] - curvature
        share = 1.0 / members
        right = right - jnp.sum(right, axis=0, keepdims=True) * share
        curvature = curvature - jnp.sum(curvature, axis=0, keepdims=True) * share
        curvature = curvature - jnp.sum(curvature, axis=1, keepdims=True) * share
        full_ref[:, 0:members] = curvature
        full_ref[:, members:width] = right
        eye = iota((members, members), 0) == iota((members, members), 1)
        bound = jnp.max(jnp.sum(jnp.abs(curvature), axis=0, keepdims=True))
        shifts = [(1.0 + lam_ref[l]) * (members - 1) for l in range(n_lam)]
        least = shifts[0]
        for shift in shifts[1:]:
            least = jnp.minimum(least, shift)
        rate = bound / (bound + 2.0 * least)
        for l in range(n_lam):
            alpha = 2.0 / (bound + 2.0 * shifts[l])
            rest = jnp.where(eye, 1.0 - alpha * shifts[l], 0.0) - alpha * curvature
            inverse_ref[l] = alpha * (jnp.where(eye, 1.0, 0.0) + rest)
            rest = rest.astype(BF16)
            power_ref[l] = dot(rest, rest).astype(BF16)

        def going(state):
            return jnp.logical_and(state[0] > 0.02, state[1] < 24)

        def squared(state):
            for l in range(n_lam):
                power = power_ref[l]
                both = jnp.concatenate([power, inverse_ref[l].astype(BF16)], axis=1)
                step = dot(power, both)
                inverse_ref[l] = inverse_ref[l] + step[:, members:width]
                power_ref[l] = step[:, 0:members].astype(BF16)
            return state[0] * state[0], state[1] + 1

        lax.while_loop(going, squared, (rate * rate, jnp.int32(0)))
        inverses = [inverse_ref[l].astype(BF16) for l in range(n_lam)]
        right_low = right.astype(BF16)
        answers = [dot(inverse, right_low) for inverse in inverses]
        high, low = halves(curvature)
        wide = jnp.concatenate([high, low], axis=1)
        sizes = []
        for _ in range(2):
            changes = []
            for l in range(0, n_lam, 2):
                pair = jnp.concatenate(answers[l : l + 2], axis=1)
                top, bottom = halves(pair)
                product = dot(wide, jnp.concatenate([top, top], axis=0)) + dot(high, bottom)
                for q in range(2):
                    part = product[:, q * members : (q + 1) * members]
                    left = right - (part + shifts[l + q] * answers[l + q])
                    changes.append(dot(inverses[l + q], left.astype(BF16)))
            answers = [a + c for a, c in zip(answers, changes)]
            sizes.append([jnp.max(jnp.abs(c), axis=0, keepdims=True) for c in changes])
        good = None
        for l in range(n_lam):
            whole = jnp.max(jnp.max(jnp.abs(answers[l]), axis=0, keepdims=True))
            first, second = jnp.max(sizes[0][l]), jnp.max(sizes[1][l])
            fine = jnp.logical_and(second <= 1e-3 * whole, second <= jnp.maximum(0.2 * first, 1e-5 * whole))
            good = fine if good is None else jnp.logical_and(good, fine)
            answer_ref[l] = answers[l]

        @pl.when(jnp.logical_not(good))
        def _():
            answer_ref[...] = jnp.zeros_like(answer_ref)

            def improve(i, carry):
                eliminate(lam_ref, full_ref, work_ref, answer_ref)
                return carry

            lax.fori_loop(0, 2, improve, 0)

        transform = answer_ref[0].astype(BF16).astype(F32)
        step = (iota((members, members), 0) - iota((members, members), 1)) % members
        for start in (1, 1 + SPREAD):
            excess = jnp.sum(transform, axis=0, keepdims=True) * (1.0 / SPREAD)
            chosen = jnp.logical_and(step >= start, step < start + SPREAD)
            moved = jnp.where(chosen, transform - excess, transform)
            transform = moved.astype(BF16).astype(F32)
        transform = transform.astype(BF16)
        for i in range(count):
            loads[i].wait()
            for at in range(0, chunk, TILE):
                x = hold_ref[i, at : at + TILE, :]
                updated = x.astype(F32) + dot(x, transform)
                made_ref[i, at : at + TILE, :] = updated.astype(BF16)
            stores[i].start()
        moments = gram_ref[...]
        top, low = halves(moments)
        rest = moments - top.astype(F32)
        middle, low = halves(rest)
        wide = jnp.concatenate([top, middle], axis=1)
        for l in range(0, n_lam, 2):
            pair = jnp.concatenate([answer_ref[l], answer_ref[l + 1]], axis=1).astype(BF16)
            spread = dot(wide, jnp.concatenate([pair, pair], axis=0)) + dot(low, pair)
            totals = jnp.sum(pair.astype(F32) * spread, axis=0, keepdims=True)
            for q in range(2):
                norm_ref[l + q : l + q + 1, :] = totals[:, q * members : (q + 1) * members]
        for store in stores:
            store.wait()

    return pl.pallas_call(
        body,
        out_shape=[
            jax.ShapeDtypeStruct((cells, members), BF16),
            jax.ShapeDtypeStruct((n_lam, members), F32),
        ],
        in_specs=[SMEM, SMEM] + [VMEM] * (n_obs + 1) + [ANY],
        out_specs=[ANY, VMEM],
        scratch_shapes=[
            pltpu.VMEM((members, width), F32),
            pltpu.VMEM((n_lam, members, width), F32),
            pltpu.VMEM((n_lam, members, members), BF16),
            pltpu.VMEM((n_lam, members, members), F32),
            pltpu.VMEM((n_lam, members, members), F32),
            pltpu.VMEM((count, chunk, members), BF16),
            pltpu.VMEM((count, chunk, members), BF16),
            pltpu.SemaphoreType.DMA((count,)),
            pltpu.SemaphoreType.DMA((count,)),
        ],
        compiler_params=params(52),
        cost_estimate=cost(2e9, 4 * cells * members),
        name="finish",
    )(place_obs, lambdas, *bands, field_gram, log_k)


def field_moments(log_k, total, first, chunk, count):
    members = log_k.shape[1]

    def body(x_ref, total_ref, out_ref, hold_ref, sem):
        copies = []
        for i in range(count):
            rows = pl.ds(first + i * chunk, chunk)
            copies.append(pltpu.make_async_copy(x_ref.at[rows], hold_ref.at[i], sem.at[i]))
            copies[i].start()
        eye = iota((members, members), 0) == iota((members, members), 1)
        centre = (jnp.where(eye, 1.0, 0.0) - 1.0 / members).astype(BF16)
        moments = total_ref[...]
        for i in range(count):
            copies[i].wait()
            anomalies = dot(hold_ref[i], centre).astype(BF16)
            moments = moments + dot(anomalies, anomalies, ((0,), (0,)))
        out_ref[...] = moments

    return pl.pallas_call(
        body,
        out_shape=jax.ShapeDtypeStruct((members, members), F32),
        in_specs=[ANY, VMEM],
        out_specs=VMEM,
        scratch_shapes=[
            pltpu.VMEM((count, chunk, members), BF16),
            pltpu.SemaphoreType.DMA((count,)),
        ],
        compiler_params=params(52),
        cost_estimate=cost(6.0e9, count * chunk * members * 2),
        name="field_moments",
    )(log_k, total)


def sum_band(gathered, after):
    n_tiles, band, width = gathered.shape

    def body(gathered_ref, after_ref, out_ref):
        total = gathered_ref[0].astype(F32)
        for t in range(1, n_tiles):
            total = total + gathered_ref[t].astype(F32)
        out_ref[...] = total

    return pl.pallas_call(
        body,
        out_shape=jax.ShapeDtypeStruct((band, width), F32),
        in_specs=[VMEM, VMEM],
        out_specs=VMEM,
        compiler_params=params(8),
        cost_estimate=cost(1e7, 1e6),
        name="sum_band",
    )(gathered, after)


def shifted(array, axis, step):
    n = lax.axis_size(axis)
    return lax.ppermute(array, axis, [(i, (i + step) % n) for i in range(n)])


def on_device(
    log_k, heads_pred, slot_well, tile_count, obs_values, obs_std, loc_blocks, taper, lambdas
):
    n_obs = lax.axis_size("obs")
    n_cell = lax.axis_size("cell")
    members = heads_pred.shape[1]
    place_obs = lax.axis_index("obs").astype(jnp.int32).reshape(1)
    sent, own_wells = send_rows(
        slot_well, tile_count, heads_pred, obs_values, obs_std, n_obs, n_cell
    )
    received = lax.all_to_all(sent, "cell", split_axis=0, concat_axis=0, tiled=True)
    wells = [own_wells] + [shifted(own_wells, "obs", k) for k in range(1, n_obs)]
    cells = log_k.shape[0]
    chunk = cells // 6
    moments = jnp.zeros((members, members), F32)
    moments = field_moments(log_k, moments, 0, chunk, 2)
    column_blocks = jnp.arange(n_obs, dtype=jnp.int32) * n_cell + lax.axis_index("cell")
    weights = jnp.sum(
        taper[:, :, None]
        * (loc_blocks[:, :, None] == column_blocks[None, None, :]).astype(F32),
        axis=1,
    )
    grams = block_grams(place_obs, received, wells, moments, n_obs)
    parts = [grams[0]] + [shifted(grams[k], "obs", k) for k in range(1, n_obs)]
    terms = tile_terms(weights, parts)
    gathered = lax.all_to_all(terms, "cell", split_axis=0, concat_axis=0, tiled=True)
    moments = field_moments(log_k, moments, 2 * chunk, chunk, 4)
    own_band = sum_band(gathered, moments)
    bands = [own_band] + [shifted(own_band, "obs", k) for k in range(1, n_obs)]
    posterior, norms = finish(place_obs, lambdas, bands, moments, log_k, 6)
    return (posterior, norms[None])


def solution(mesh):
    return jax.shard_map(
        on_device,
        mesh=mesh,
        in_specs=(
            P(("obs", "cell"), None),
            P(("obs", "cell"), None),
            P(("obs", "cell")),
            P(("obs", "cell")),
            P(("obs", "cell"), None),
            P(("obs", "cell")),
            P(),
            P(),
            P(),
        ),
        out_specs=(P(("obs", "cell"), None), P(("obs", "cell"), None, None)),
        check_vma=False,
    )
```

```python
import jax
import jax.numpy as jnp
from jax import lax
from jax.experimental import pallas as pl
from jax.experimental.pallas import tpu as pltpu
from jax.sharding import PartitionSpec as P


CAP = 16
EXTRA = 8
SPREAD = 16
TILE = 512
F32 = jnp.float32
BF16 = jnp.bfloat16
HIGHEST = lax.Precision.HIGHEST
SMEM = pl.BlockSpec(memory_space=pltpu.SMEM)
VMEM = pl.BlockSpec(memory_space=pltpu.VMEM)
ANY = pl.BlockSpec(memory_space=pl.ANY)
MIB = 1 << 20


def iota(shape, dim):
    return lax.broadcasted_iota(jnp.int32, shape, dim)


def one_hot(cond):
    return jnp.where(cond, 1.0, 0.0).astype(BF16)


def dot(a, b, contract=((1,), (0,)), precision=None):
    return lax.dot_general(
        a, b, (contract, ((), ())), precision=precision, preferred_element_type=F32
    )


def params(mib):
    return pltpu.CompilerParams(vmem_limit_bytes=mib * MIB)


def cost(flops, size):
    return pl.CostEstimate(flops=int(flops), bytes_accessed=int(size), transcendentals=0)


def send_rows(slot_well, tile_count, heads, obs_values, obs_std, n_obs, n_cell):
    slots, members = heads.shape
    wells_dev = obs_values.shape[0]
    rows = n_obs * CAP

    def body(count_ref, well_ref, heads_ref, value_ref, std_ref, out_ref, join_ref):
        well = well_ref[...]
        valid = iota((1, slots), 1) < count_ref[0]
        block = jnp.where(valid, well // wells_dev, -1)
        place = well % wells_dev
        hits = one_hot(iota((n_obs * n_cell, slots), 0) == block)
        before = one_hot(iota((slots, slots), 0) < iota((slots, slots), 1))
        rank = jnp.sum(dot(hits, before) * hits.astype(F32), axis=0, keepdims=True)
        row = (block // n_cell) * CAP + rank.astype(jnp.int32)
        column = jnp.where(valid, block % n_cell, -1)
        target = jnp.where(valid, column * rows + row, -1)
        marks = jnp.where(iota((n_cell, slots), 0) == column, place + 1, 0)
        marks = marks.astype(F32).astype(BF16)
        places = dot(marks, one_hot(iota((members, slots), 0) == row), ((1,), (1,)))
        values = heads_ref[...]
        for c in range(n_cell):
            pick = one_hot(iota((rows, slots), 0) + c * rows == target)
            out_ref[c, 0:rows, :] = dot(pick, values).astype(BF16)
            out_ref[c, rows : rows + EXTRA, :] = jnp.broadcast_to(
                places[c : c + 1, :], (EXTRA, members)
            ).astype(BF16)
        join_ref[0:wells_dev, :] = value_ref[...]
        join_ref[wells_dev:, :] = jnp.broadcast_to(std_ref[...], (EXTRA, wells_dev))

    return pl.pallas_call(
        body,
        out_shape=[
            jax.ShapeDtypeStruct((n_cell, rows + EXTRA, members), BF16),
            jax.ShapeDtypeStruct((wells_dev + EXTRA, members), F32),
        ],
        in_specs=[SMEM] + [VMEM] * 4,
        out_specs=[VMEM, VMEM],
        compiler_params=params(60),
        cost_estimate=cost(1e9, 1e6),
        name="send_rows",
    )(tile_count, slot_well.reshape(1, slots), heads, obs_values, obs_std.reshape(1, wells_dev))


def block_grams(place_obs, received, wells, after, n_obs):
    sources, _, members = received.shape
    rows = n_obs * CAP
    slots = sources * CAP
    wells_dev = wells[0].shape[0] - EXTRA
    band = members // n_obs

    def body(me_ref, recv_ref, after_ref, *refs):
        well_refs, out_refs, gram_ref = refs[:n_obs], refs[n_obs : 2 * n_obs], refs[-1]
        me = me_ref[0]
        tail = recv_ref[:, rows : rows + EXTRA, :].astype(F32)
        places = jnp.max(tail, axis=1).astype(BF16)
        mine = iota((sources, slots), 0) == iota((sources, slots), 1) // CAP
        eye = iota((wells_dev, wells_dev), 0) == iota((wells_dev, wells_dev), 1)
        for k in range(n_obs):
            owner = lax.rem(me - k + n_obs, n_obs)
            first = owner * CAP
            spread = one_hot(
                iota((members, slots), 0) == iota((members, slots), 1) % CAP + first
            )
            spot = jnp.where(mine, dot(places, spread), 0.0)
            spot = jnp.sum(spot, axis=0, keepdims=True).astype(jnp.int32)
            pick = one_hot(iota((wells_dev, slots), 0) + 1 == spot)
            heads = recv_ref[:, pl.ds(pl.multiple_of(first, CAP), CAP), :]
            predicted = dot(pick, heads.reshape(slots, members))
            mean = jnp.sum(predicted, axis=1, keepdims=True) * (1.0 / members)
            deviation = well_refs[k][wells_dev : wells_dev + 1, :]
            deviation = jnp.sum(jnp.where(eye, deviation, 0.0), axis=1, keepdims=True)
            scale = 1.0 / deviation
            scaled = (predicted - mean) * scale
            offset = (well_refs[k][0:wells_dev, :] - mean) * scale
            joined = jnp.concatenate([scaled, offset], axis=1)
            gram_ref[...] = dot(scaled.T, joined, precision=HIGHEST)
            for step in range(n_obs):
                dest = lax.rem(me + step, n_obs)
                part = gram_ref[pl.ds(pl.multiple_of(dest * band, band), band), :]
                out_refs[step][owner] = part.astype(BF16)

    return pl.pallas_call(
        body,
        out_shape=[jax.ShapeDtypeStruct((n_obs, band, 2 * members), BF16)] * n_obs,
        in_specs=[SMEM] + [VMEM] * (2 + n_obs),
        out_specs=[VMEM] * n_obs,
        scratch_shapes=[pltpu.VMEM((members, 2 * members), F32)],
        compiler_params=params(16),
        cost_estimate=cost(1e9, 1e6),
        name="block_grams",
    )(place_obs, received, after, *wells)


def tile_terms(weights, parts):
    n_tiles, n_obs = weights.shape
    _, band, width = parts[0].shape

    def body(weight_ref, *refs):
        out_ref = refs[-1]
        totals = []
        for o in range(n_obs):
            total = refs[0][o].astype(F32)
            for ref in refs[1:-1]:
                total = total + ref[o].astype(F32)
            totals.append(total)
        for t in range(n_tiles):
            term = weight_ref[t, 0] * totals[0]
            for o in range(1, n_obs):
                term = term + weight_ref[t, o] * totals[o]
            out_ref[t] = term.astype(BF16)

    return pl.pallas_call(
        body,
        out_shape=jax.ShapeDtypeStruct((n_tiles, band, width), BF16),
        in_specs=[SMEM] + [VMEM] * len(parts),
        out_specs=VMEM,
        compiler_params=params(16),
        cost_estimate=cost(1e8, 1e6),
        name="tile_terms",
    )(weights, *parts)


def invert_packed(packed, size, groups):
    lanes = size * groups
    lane = iota((size, lanes), 1)
    row = iota((size, lanes), 0)
    for j in range(size):
        column = jnp.take_along_axis(
            packed, lane // size * size + j, axis=1, mode="promise_in_bounds"
        )
        inverse = 1.0 / column[j : j + 1, :]
        pivot_row = packed[j : j + 1, :] * inverse
        here = lane % size == j
        others = jnp.where(here, -(column * inverse), packed - column * pivot_row)
        packed = jnp.where(row == j, jnp.where(here, inverse, pivot_row), others)
    return packed


def halves(a):
    high = a.astype(BF16)
    return high, (a - high.astype(F32)).astype(BF16)


def finish(place_obs, lambdas, bands, field_gram, log_k, count):
    n_obs = len(bands)
    band, width = bands[0].shape
    members = width // 2
    n_lam = lambdas.shape[0]
    size = members // n_lam
    cells = log_k.shape[0]
    chunk = cells // count

    def eliminate(lam_ref, full_ref, work_ref, answer_ref):
        eye = iota((members, members), 0) == iota((members, members), 1)
        for l in range(n_lam):
            shift = (1.0 + lam_ref[l]) * (members - 1)
            system = full_ref[:, 0:members] + jnp.where(eye, shift, 0.0)
            known = dot(system, answer_ref[l], precision=HIGHEST)
            work_ref[l, :, 0:members] = system
            work_ref[l, :, members:width] = full_ref[:, members:width] - known
        lane = iota((size, members), 1)
        tall_lane = iota((members, members), 1)
        for kb in range(members // size):
            at = kb * size
            packed = jnp.zeros((size, members), F32)
            for l in range(n_lam):
                piece = work_ref[l, at : at + size, 0:members]
                turn = (l - kb) * size % members
                piece = pltpu.roll(piece, turn, 1) if turn else piece
                packed = jnp.where(lane // size == l, piece, packed)
            packed = invert_packed(packed, size, n_lam)
            diag = jnp.concatenate(
                [jnp.where(lane // size == l, packed, 0.0) for l in range(n_lam)], axis=0
            )
            rows = jnp.concatenate(
                [work_ref[l, at : at + size, :] for l in range(n_lam)], axis=0
            )
            upper = dot(diag, rows, precision=HIGHEST)
            left = []
            for l in range(n_lam):
                piece = work_ref[l, :, 0:members]
                turn = (l - kb) * size % members
                piece = pltpu.roll(piece, turn, 1) if turn else piece
                left.append(jnp.where(tall_lane // size == l, piece, 0.0))
            delta = dot(jnp.concatenate(left, axis=0), upper, precision=HIGHEST)
            for l in range(n_lam):
                work_ref[l] = work_ref[l] - delta[l * members : (l + 1) * members, :]
                work_ref[l, at : at + size, :] = upper[l * size : (l + 1) * size, :]
        for l in range(n_lam):
            answer_ref[l] = answer_ref[l] + work_ref[l, :, members:width]

    def body(me_ref, lam_ref, *refs):
        band_refs = refs[:n_obs]
        gram_ref, field_ref, out_ref, norm_ref = refs[n_obs : n_obs + 4]
        full_ref, work_ref, power_ref, inverse_ref, answer_ref = refs[n_obs + 4 : n_obs + 9]
        hold_ref, made_ref, in_sem, out_sem = refs[n_obs + 9 :]
        loads, stores = [], []
        for i in range(count):
            rows = pl.ds(i * chunk, chunk)
            loads.append(pltpu.make_async_copy(field_ref.at[rows], hold_ref.at[i], in_sem.at[i]))
            stores.append(pltpu.make_async_copy(made_ref.at[i], out_ref.at[rows], out_sem.at[i]))
            loads[i].start()
        me = me_ref[0]
        for k in range(n_obs):
            owner = lax.rem(me - k + n_obs, n_obs)
            rows = pl.ds(pl.multiple_of(owner * band, band), band)
            full_ref[rows, :] = band_refs[k][...]
        curvature = full_ref[:, 0:members]
        right = full_ref[:, members:width] - curvature
        share = 1.0 / members
        right = right - jnp.sum(right, axis=0, keepdims=True) * share
        curvature = curvature - jnp.sum(curvature, axis=0, keepdims=True) * share
        curvature = curvature - jnp.sum(curvature, axis=1, keepdims=True) * share
        full_ref[:, 0:members] = curvature
        full_ref[:, members:width] = right
        eye = iota((members, members), 0) == iota((members, members), 1)
        bound = jnp.max(jnp.sum(jnp.abs(curvature), axis=0, keepdims=True))
        shifts = [(1.0 + lam_ref[l]) * (members - 1) for l in range(n_lam)]
        least = shifts[0]
        for shift in shifts[1:]:
            least = jnp.minimum(least, shift)
        rate = bound / (bound + 2.0 * least)
        for l in range(n_lam):
            alpha = 2.0 / (bound + 2.0 * shifts[l])
            rest = jnp.where(eye, 1.0 - alpha * shifts[l], 0.0) - alpha * curvature
            inverse_ref[l] = alpha * (jnp.where(eye, 1.0, 0.0) + rest)
            rest = rest.astype(BF16)
            power_ref[l] = dot(rest, rest).astype(BF16)

        def going(state):
            return jnp.logical_and(state[0] > 0.02, state[1] < 24)

        def squared(state):
            for l in range(n_lam):
                power = power_ref[l]
                both = jnp.concatenate([power, inverse_ref[l].astype(BF16)], axis=1)
                step = dot(power, both)
                inverse_ref[l] = inverse_ref[l] + step[:, members:width]
                power_ref[l] = step[:, 0:members].astype(BF16)
            return state[0] * state[0], state[1] + 1

        lax.while_loop(going, squared, (rate * rate, jnp.int32(0)))
        inverses = [inverse_ref[l].astype(BF16) for l in range(n_lam)]
        right_low = right.astype(BF16)
        answers = [dot(inverse, right_low) for inverse in inverses]
        high, low = halves(curvature)
        wide = jnp.concatenate([high, low], axis=1)
        sizes = []
        for _ in range(2):
            changes = []
            for l in range(0, n_lam, 2):
                pair = jnp.concatenate(answers[l : l + 2], axis=1)
                top, bottom = halves(pair)
                product = dot(wide, jnp.concatenate([top, top], axis=0)) + dot(high, bottom)
                for q in range(2):
                    part = product[:, q * members : (q + 1) * members]
                    left = right - (part + shifts[l + q] * answers[l + q])
                    changes.append(dot(inverses[l + q], left.astype(BF16)))
            answers = [a + c for a, c in zip(answers, changes)]
            sizes.append([jnp.max(jnp.abs(c), axis=0, keepdims=True) for c in changes])
        good = None
        for l in range(n_lam):
            whole = jnp.max(jnp.max(jnp.abs(answers[l]), axis=0, keepdims=True))
            first, second = jnp.max(sizes[0][l]), jnp.max(sizes[1][l])
            fine = jnp.logical_and(second <= 1e-3 * whole, second <= jnp.maximum(0.2 * first, 1e-5 * whole))
            good = fine if good is None else jnp.logical_and(good, fine)
            answer_ref[l] = answers[l]

        @pl.when(jnp.logical_not(good))
        def _():
            answer_ref[...] = jnp.zeros_like(answer_ref)

            def improve(i, carry):
                eliminate(lam_ref, full_ref, work_ref, answer_ref)
                return carry

            lax.fori_loop(0, 2, improve, 0)

        transform = answer_ref[0].astype(BF16).astype(F32)
        step = (iota((members, members), 0) - iota((members, members), 1)) % members
        for start in (1, 1 + SPREAD):
            excess = jnp.sum(transform, axis=0, keepdims=True) * (1.0 / SPREAD)
            chosen = jnp.logical_and(step >= start, step < start + SPREAD)
            moved = jnp.where(chosen, transform - excess, transform)
            transform = moved.astype(BF16).astype(F32)
        transform = transform.astype(BF16)
        for i in range(count):
            loads[i].wait()
            for at in range(0, chunk, TILE):
                x = hold_ref[i, at : at + TILE, :]
                updated = x.astype(F32) + dot(x, transform)
                made_ref[i, at : at + TILE, :] = updated.astype(BF16)
            stores[i].start()
        moments = gram_ref[...]
        top, low = halves(moments)
        rest = moments - top.astype(F32)
        middle, low = halves(rest)
        wide = jnp.concatenate([top, middle], axis=1)
        for l in range(0, n_lam, 2):
            pair = jnp.concatenate([answer_ref[l], answer_ref[l + 1]], axis=1).astype(BF16)
            spread = dot(wide, jnp.concatenate([pair, pair], axis=0)) + dot(low, pair)
            totals = jnp.sum(pair.astype(F32) * spread, axis=0, keepdims=True)
            for q in range(2):
                norm_ref[l + q : l + q + 1, :] = totals[:, q * members : (q + 1) * members]
        for store in stores:
            store.wait()

    return pl.pallas_call(
        body,
        out_shape=[
            jax.ShapeDtypeStruct((cells, members), BF16),
            jax.ShapeDtypeStruct((n_lam, members), F32),
        ],
        in_specs=[SMEM, SMEM] + [VMEM] * (n_obs + 1) + [ANY],
        out_specs=[ANY, VMEM],
        scratch_shapes=[
            pltpu.VMEM((members, width), F32),
            pltpu.VMEM((n_lam, members, width), F32),
            pltpu.VMEM((n_lam, members, members), BF16),
            pltpu.VMEM((n_lam, members, members), F32),
            pltpu.VMEM((n_lam, members, members), F32),
            pltpu.VMEM((count, chunk, members), BF16),
            pltpu.VMEM((count, chunk, members), BF16),
            pltpu.SemaphoreType.DMA((count,)),
            pltpu.SemaphoreType.DMA((count,)),
        ],
        compiler_params=params(52),
        cost_estimate=cost(2e9, 4 * cells * members),
        name="finish",
    )(place_obs, lambdas, *bands, field_gram, log_k)


def field_moments(log_k, total, first, chunk, count):
    members = log_k.shape[1]

    def body(x_ref, total_ref, out_ref, hold_ref, sem):
        copies = []
        for i in range(count):
            rows = pl.ds(first + i * chunk, chunk)
            copies.append(pltpu.make_async_copy(x_ref.at[rows], hold_ref.at[i], sem.at[i]))
            copies[i].start()
        eye = iota((members, members), 0) == iota((members, members), 1)
        centre = (jnp.where(eye, 1.0, 0.0) - 1.0 / members).astype(BF16)
        moments = total_ref[...]
        for i in range(count):
            copies[i].wait()
            anomalies = dot(hold_ref[i], centre).astype(BF16)
            moments = moments + dot(anomalies, anomalies, ((0,), (0,)))
        out_ref[...] = moments

    return pl.pallas_call(
        body,
        out_shape=jax.ShapeDtypeStruct((members, members), F32),
        in_specs=[ANY, VMEM],
        out_specs=VMEM,
        scratch_shapes=[
            pltpu.VMEM((count, chunk, members), BF16),
            pltpu.SemaphoreType.DMA((count,)),
        ],
        compiler_params=params(52),
        cost_estimate=cost(6.0e9, count * chunk * members * 2),
        name="field_moments",
    )(log_k, total)


def sum_band(gathered, after):
    n_tiles, band, width = gathered.shape

    def body(gathered_ref, after_ref, out_ref):
        total = gathered_ref[0].astype(F32)
        for t in range(1, n_tiles):
            total = total + gathered_ref[t].astype(F32)
        out_ref[...] = total

    return pl.pallas_call(
        body,
        out_shape=jax.ShapeDtypeStruct((band, width), F32),
        in_specs=[VMEM, VMEM],
        out_specs=VMEM,
        compiler_params=params(8),
        cost_estimate=cost(1e7, 1e6),
        name="sum_band",
    )(gathered, after)


def shifted(array, axis, step):
    n = lax.axis_size(axis)
    return lax.ppermute(array, axis, [(i, (i + step) % n) for i in range(n)])


def exchanged(arrays):
    moved = []
    for k, array in enumerate(arrays, 1):
        moved.append(shifted(array, "obs", k))
    return moved


def on_device(
    log_k, heads_pred, slot_well, tile_count, obs_values, obs_std, loc_blocks, taper, lambdas
):
    n_obs = lax.axis_size("obs")
    n_cell = lax.axis_size("cell")
    members = heads_pred.shape[1]
    place_obs = lax.axis_index("obs").astype(jnp.int32).reshape(1)
    sent, own_wells = send_rows(
        slot_well, tile_count, heads_pred, obs_values, obs_std, n_obs, n_cell
    )
    received = lax.all_to_all(sent, "cell", split_axis=0, concat_axis=0, tiled=True)
    wells = [own_wells] + [shifted(own_wells, "obs", k) for k in range(1, n_obs)]
    cells = log_k.shape[0]
    chunk = cells // 6
    moments = jnp.zeros((members, members), F32)
    moments = field_moments(log_k, moments, 0, chunk, 2)
    column_blocks = jnp.arange(n_obs, dtype=jnp.int32) * n_cell + lax.axis_index("cell")
    weights = jnp.sum(
        taper[:, :, None]
        * (loc_blocks[:, :, None] == column_blocks[None, None, :]).astype(F32),
        axis=1,
    )
    grams = block_grams(place_obs, received, wells, moments, n_obs)
    parts = [grams[0]] + exchanged(grams[1:])
    terms = tile_terms(weights, parts)
    gathered = lax.all_to_all(terms, "cell", split_axis=0, concat_axis=0, tiled=True)
    moments = field_moments(log_k, moments, 2 * chunk, chunk, 4)
    own_band = sum_band(gathered, moments)
    bands = [own_band] + exchanged([own_band] * (n_obs - 1))
    posterior, norms = finish(place_obs, lambdas, bands, moments, log_k, 6)
    return (posterior, norms[None])


def solution(mesh):
    return jax.shard_map(
        on_device,
        mesh=mesh,
        in_specs=(
            P(("obs", "cell"), None),
            P(("obs", "cell"), None),
            P(("obs", "cell")),
            P(("obs", "cell")),
            P(("obs", "cell"), None),
            P(("obs", "cell")),
            P(),
            P(),
            P(),
        ),
        out_specs=(P(("obs", "cell"), None), P(("obs", "cell"), None, None)),
        check_vma=False,
    )
```

```python
import jax
import jax.numpy as jnp
from jax import lax
from jax.experimental import pallas as pl
from jax.experimental.pallas import tpu as pltpu
from jax.sharding import PartitionSpec as P


CAP = 16
EXTRA = 8
SPREAD = 16
TILE = 512
PARTS = 2
F32 = jnp.float32
BF16 = jnp.bfloat16
HIGHEST = lax.Precision.HIGHEST
SMEM = pl.BlockSpec(memory_space=pltpu.SMEM)
VMEM = pl.BlockSpec(memory_space=pltpu.VMEM)
ANY = pl.BlockSpec(memory_space=pl.ANY)
MIB = 1 << 20


def iota(shape, dim):
    return lax.broadcasted_iota(jnp.int32, shape, dim)


def one_hot(cond):
    return jnp.where(cond, 1.0, 0.0).astype(BF16)


def dot(a, b, contract=((1,), (0,)), precision=None):
    return lax.dot_general(
        a, b, (contract, ((), ())), precision=precision, preferred_element_type=F32
    )


def params(mib):
    return pltpu.CompilerParams(vmem_limit_bytes=mib * MIB)


def cost(flops, size):
    return pl.CostEstimate(flops=int(flops), bytes_accessed=int(size), transcendentals=0)


def in_parts(source, target, sem):
    length = source.shape[0] // PARTS
    spans = [pl.ds(i * length, length) for i in range(PARTS)]
    return [
        pltpu.make_async_copy(source.at[span], target.at[span], sem.at[i])
        for i, span in enumerate(spans)
    ]


def send_rows(slot_well, tile_count, heads, obs_values, obs_std, n_obs, n_cell):
    slots, members = heads.shape
    wells_dev = obs_values.shape[0]
    rows = n_obs * CAP

    def body(count_ref, well_ref, heads_ref, value_ref, std_ref, out_ref, join_ref, hold_ref, sem):
        copies = in_parts(hold_ref, out_ref, sem)
        well = well_ref[...]
        valid = iota((1, slots), 1) < count_ref[0]
        block = jnp.where(valid, well // wells_dev, -1)
        place = well % wells_dev
        hits = one_hot(iota((n_obs * n_cell, slots), 0) == block)
        before = one_hot(iota((slots, slots), 0) < iota((slots, slots), 1))
        rank = jnp.sum(dot(hits, before) * hits.astype(F32), axis=0, keepdims=True)
        row = (block // n_cell) * CAP + rank.astype(jnp.int32)
        column = jnp.where(valid, block % n_cell, -1)
        target = jnp.where(valid, column * rows + row, -1)
        marks = jnp.where(iota((n_cell, slots), 0) == column, place + 1, 0)
        marks = marks.astype(F32).astype(BF16)
        places = dot(marks, one_hot(iota((members, slots), 0) == row), ((1,), (1,)))
        values = heads_ref[...]
        for c in range(n_cell):
            pick = one_hot(iota((rows, slots), 0) + c * rows == target)
            hold_ref[c, 0:rows, :] = dot(pick, values).astype(BF16)
            hold_ref[c, rows : rows + EXTRA, :] = jnp.broadcast_to(
                places[c : c + 1, :], (EXTRA, members)
            ).astype(BF16)
            if (c + 1) % (n_cell // PARTS) == 0:
                copies[c // (n_cell // PARTS)].start()
        join_ref[0:wells_dev, :] = value_ref[...]
        join_ref[wells_dev:, :] = jnp.broadcast_to(std_ref[...], (EXTRA, wells_dev))
        for copy in copies:
            copy.wait()

    return pl.pallas_call(
        body,
        out_shape=[
            jax.ShapeDtypeStruct((n_cell, rows + EXTRA, members), BF16),
            jax.ShapeDtypeStruct((wells_dev + EXTRA, members), F32),
        ],
        in_specs=[SMEM] + [VMEM] * 4,
        out_specs=[ANY, VMEM],
        scratch_shapes=[
            pltpu.VMEM((n_cell, rows + EXTRA, members), BF16),
            pltpu.SemaphoreType.DMA((PARTS,)),
        ],
        compiler_params=params(60),
        cost_estimate=cost(1e9, 1e6),
        name="send_rows",
    )(tile_count, slot_well.reshape(1, slots), heads, obs_values, obs_std.reshape(1, wells_dev))


def block_grams(place_obs, received, wells, after, n_obs):
    sources, _, members = received.shape
    rows = n_obs * CAP
    slots = sources * CAP
    wells_dev = wells[0].shape[0] - EXTRA
    band = members // n_obs

    def body(me_ref, recv_ref, after_ref, *refs):
        well_refs, out_refs, gram_ref = refs[:n_obs], refs[n_obs : 2 * n_obs], refs[-1]
        me = me_ref[0]
        tail = recv_ref[:, rows : rows + EXTRA, :].astype(F32)
        places = jnp.max(tail, axis=1).astype(BF16)
        mine = iota((sources, slots), 0) == iota((sources, slots), 1) // CAP
        eye = iota((wells_dev, wells_dev), 0) == iota((wells_dev, wells_dev), 1)
        for k in range(n_obs):
            owner = lax.rem(me - k + n_obs, n_obs)
            first = owner * CAP
            spread = one_hot(
                iota((members, slots), 0) == iota((members, slots), 1) % CAP + first
            )
            spot = jnp.where(mine, dot(places, spread), 0.0)
            spot = jnp.sum(spot, axis=0, keepdims=True).astype(jnp.int32)
            pick = one_hot(iota((wells_dev, slots), 0) + 1 == spot)
            heads = recv_ref[:, pl.ds(pl.multiple_of(first, CAP), CAP), :]
            predicted = dot(pick, heads.reshape(slots, members))
            mean = jnp.sum(predicted, axis=1, keepdims=True) * (1.0 / members)
            deviation = well_refs[k][wells_dev : wells_dev + 1, :]
            deviation = jnp.sum(jnp.where(eye, deviation, 0.0), axis=1, keepdims=True)
            scale = 1.0 / deviation
            scaled = (predicted - mean) * scale
            offset = (well_refs[k][0:wells_dev, :] - mean) * scale
            joined = jnp.concatenate([scaled, offset], axis=1)
            gram_ref[...] = dot(scaled.T, joined, precision=HIGHEST)
            for step in range(n_obs):
                dest = lax.rem(me + step, n_obs)
                part = gram_ref[pl.ds(pl.multiple_of(dest * band, band), band), :]
                out_refs[step][owner] = part.astype(BF16)

    return pl.pallas_call(
        body,
        out_shape=[jax.ShapeDtypeStruct((n_obs, band, 2 * members), BF16)] * n_obs,
        in_specs=[SMEM] + [VMEM] * (2 + n_obs),
        out_specs=[VMEM] * n_obs,
        scratch_shapes=[pltpu.VMEM((members, 2 * members), F32)],
        compiler_params=params(16),
        cost_estimate=cost(1e9, 1e6),
        name="block_grams",
    )(place_obs, received, after, *wells)


def tile_terms(weights, parts):
    n_tiles, n_obs = weights.shape
    _, band, width = parts[0].shape

    def body(weight_ref, *refs):
        out_ref, hold_ref, sem = refs[-3:]
        copies = in_parts(hold_ref, out_ref, sem)
        totals = []
        for o in range(n_obs):
            total = refs[0][o].astype(F32)
            for ref in refs[1:-3]:
                total = total + ref[o].astype(F32)
            totals.append(total)
        for t in range(n_tiles):
            term = weight_ref[t, 0] * totals[0]
            for o in range(1, n_obs):
                term = term + weight_ref[t, o] * totals[o]
            hold_ref[t] = term.astype(BF16)
            if (t + 1) % (n_tiles // PARTS) == 0:
                copies[t // (n_tiles // PARTS)].start()
        for copy in copies:
            copy.wait()

    return pl.pallas_call(
        body,
        out_shape=jax.ShapeDtypeStruct((n_tiles, band, width), BF16),
        in_specs=[SMEM] + [VMEM] * len(parts),
        out_specs=ANY,
        scratch_shapes=[
            pltpu.VMEM((n_tiles, band, width), BF16),
            pltpu.SemaphoreType.DMA((PARTS,)),
        ],
        compiler_params=params(16),
        cost_estimate=cost(1e8, 1e6),
        name="tile_terms",
    )(weights, *parts)


def invert_packed(packed, size, groups):
    lanes = size * groups
    lane = iota((size, lanes), 1)
    row = iota((size, lanes), 0)
    for j in range(size):
        column = jnp.take_along_axis(
            packed, lane // size * size + j, axis=1, mode="promise_in_bounds"
        )
        inverse = 1.0 / column[j : j + 1, :]
        pivot_row = packed[j : j + 1, :] * inverse
        here = lane % size == j
        others = jnp.where(here, -(column * inverse), packed - column * pivot_row)
        packed = jnp.where(row == j, jnp.where(here, inverse, pivot_row), others)
    return packed


def halves(a):
    high = a.astype(BF16)
    return high, (a - high.astype(F32)).astype(BF16)


def finish(place_obs, lambdas, bands, field_gram, log_k, count):
    n_obs = len(bands)
    band, width = bands[0].shape
    members = width // 2
    n_lam = lambdas.shape[0]
    size = members // n_lam
    cells = log_k.shape[0]
    chunk = cells // count

    def eliminate(lam_ref, full_ref, work_ref, answer_ref):
        eye = iota((members, members), 0) == iota((members, members), 1)
        for l in range(n_lam):
            shift = (1.0 + lam_ref[l]) * (members - 1)
            system = full_ref[:, 0:members] + jnp.where(eye, shift, 0.0)
            known = dot(system, answer_ref[l], precision=HIGHEST)
            work_ref[l, :, 0:members] = system
            work_ref[l, :, members:width] = full_ref[:, members:width] - known
        lane = iota((size, members), 1)
        tall_lane = iota((members, members), 1)
        for kb in range(members // size):
            at = kb * size
            packed = jnp.zeros((size, members), F32)
            for l in range(n_lam):
                piece = work_ref[l, at : at + size, 0:members]
                turn = (l - kb) * size % members
                piece = pltpu.roll(piece, turn, 1) if turn else piece
                packed = jnp.where(lane // size == l, piece, packed)
            packed = invert_packed(packed, size, n_lam)
            diag = jnp.concatenate(
                [jnp.where(lane // size == l, packed, 0.0) for l in range(n_lam)], axis=0
            )
            rows = jnp.concatenate(
                [work_ref[l, at : at + size, :] for l in range(n_lam)], axis=0
            )
            upper = dot(diag, rows, precision=HIGHEST)
            left = []
            for l in range(n_lam):
                piece = work_ref[l, :, 0:members]
                turn = (l - kb) * size % members
                piece = pltpu.roll(piece, turn, 1) if turn else piece
                left.append(jnp.where(tall_lane // size == l, piece, 0.0))
            delta = dot(jnp.concatenate(left, axis=0), upper, precision=HIGHEST)
            for l in range(n_lam):
                work_ref[l] = work_ref[l] - delta[l * members : (l + 1) * members, :]
                work_ref[l, at : at + size, :] = upper[l * size : (l + 1) * size, :]
        for l in range(n_lam):
            answer_ref[l] = answer_ref[l] + work_ref[l, :, members:width]

    def body(me_ref, lam_ref, *refs):
        band_refs = refs[:n_obs]
        gram_ref, field_ref, out_ref, norm_ref = refs[n_obs : n_obs + 4]
        full_ref, work_ref, power_ref, inverse_ref, answer_ref = refs[n_obs + 4 : n_obs + 9]
        hold_ref, made_ref, in_sem, out_sem = refs[n_obs + 9 :]
        loads, stores = [], []
        for i in range(count):
            rows = pl.ds(i * chunk, chunk)
            loads.append(pltpu.make_async_copy(field_ref.at[rows], hold_ref.at[i], in_sem.at[i]))
            stores.append(pltpu.make_async_copy(made_ref.at[i], out_ref.at[rows], out_sem.at[i]))
            loads[i].start()
        me = me_ref[0]
        for k in range(n_obs):
            owner = lax.rem(me - k + n_obs, n_obs)
            rows = pl.ds(pl.multiple_of(owner * band, band), band)
            full_ref[rows, :] = band_refs[k][...]
        curvature = full_ref[:, 0:members]
        right = full_ref[:, members:width] - curvature
        share = 1.0 / members
        right = right - jnp.sum(right, axis=0, keepdims=True) * share
        curvature = curvature - jnp.sum(curvature, axis=0, keepdims=True) * share
        curvature = curvature - jnp.sum(curvature, axis=1, keepdims=True) * share
        full_ref[:, 0:members] = curvature
        full_ref[:, members:width] = right
        eye = iota((members, members), 0) == iota((members, members), 1)
        bound = jnp.max(jnp.sum(jnp.abs(curvature), axis=0, keepdims=True))
        shifts = [(1.0 + lam_ref[l]) * (members - 1) for l in range(n_lam)]
        least = shifts[0]
        for shift in shifts[1:]:
            least = jnp.minimum(least, shift)
        rate = bound / (bound + 2.0 * least)
        for l in range(n_lam):
            alpha = 2.0 / (bound + 2.0 * shifts[l])
            rest = jnp.where(eye, 1.0 - alpha * shifts[l], 0.0) - alpha * curvature
            inverse_ref[l] = alpha * (jnp.where(eye, 1.0, 0.0) + rest)
            rest = rest.astype(BF16)
            power_ref[l] = dot(rest, rest).astype(BF16)

        def going(state):
            return jnp.logical_and(state[0] > 0.02, state[1] < 24)

        def squared(state):
            for l in range(n_lam):
                power = power_ref[l]
                both = jnp.concatenate([power, inverse_ref[l].astype(BF16)], axis=1)
                step = dot(power, both)
                inverse_ref[l] = inverse_ref[l] + step[:, members:width]
                power_ref[l] = step[:, 0:members].astype(BF16)
            return state[0] * state[0], state[1] + 1

        lax.while_loop(going, squared, (rate * rate, jnp.int32(0)))
        inverses = [inverse_ref[l].astype(BF16) for l in range(n_lam)]
        right_low = right.astype(BF16)
        answers = [dot(inverse, right_low) for inverse in inverses]
        high, low = halves(curvature)
        wide = jnp.concatenate([high, low], axis=1)
        sizes = []
        for _ in range(2):
            changes = []
            for l in range(0, n_lam, 2):
                pair = jnp.concatenate(answers[l : l + 2], axis=1)
                top, bottom = halves(pair)
                product = dot(wide, jnp.concatenate([top, top], axis=0)) + dot(high, bottom)
                for q in range(2):
                    part = product[:, q * members : (q + 1) * members]
                    left = right - (part + shifts[l + q] * answers[l + q])
                    changes.append(dot(inverses[l + q], left.astype(BF16)))
            answers = [a + c for a, c in zip(answers, changes)]
            sizes.append([jnp.max(jnp.abs(c), axis=0, keepdims=True) for c in changes])
        good = None
        for l in range(n_lam):
            whole = jnp.max(jnp.max(jnp.abs(answers[l]), axis=0, keepdims=True))
            first, second = jnp.max(sizes[0][l]), jnp.max(sizes[1][l])
            fine = jnp.logical_and(second <= 1e-3 * whole, second <= jnp.maximum(0.2 * first, 1e-5 * whole))
            good = fine if good is None else jnp.logical_and(good, fine)
            answer_ref[l] = answers[l]

        @pl.when(jnp.logical_not(good))
        def _():
            answer_ref[...] = jnp.zeros_like(answer_ref)

            def improve(i, carry):
                eliminate(lam_ref, full_ref, work_ref, answer_ref)
                return carry

            lax.fori_loop(0, 2, improve, 0)

        transform = answer_ref[0].astype(BF16).astype(F32)
        step = (iota((members, members), 0) - iota((members, members), 1)) % members
        for start in (1, 1 + SPREAD):
            excess = jnp.sum(transform, axis=0, keepdims=True) * (1.0 / SPREAD)
            chosen = jnp.logical_and(step >= start, step < start + SPREAD)
            moved = jnp.where(chosen, transform - excess, transform)
            transform = moved.astype(BF16).astype(F32)
        transform = transform.astype(BF16)
        for i in range(count):
            loads[i].wait()
            for at in range(0, chunk, TILE):
                x = hold_ref[i, at : at + TILE, :]
                updated = x.astype(F32) + dot(x, transform)
                made_ref[i, at : at + TILE, :] = updated.astype(BF16)
            stores[i].start()
        moments = gram_ref[...]
        top, low = halves(moments)
        rest = moments - top.astype(F32)
        middle, low = halves(rest)
        wide = jnp.concatenate([top, middle], axis=1)
        for l in range(0, n_lam, 2):
            pair = jnp.concatenate([answer_ref[l], answer_ref[l + 1]], axis=1).astype(BF16)
            spread = dot(wide, jnp.concatenate([pair, pair], axis=0)) + dot(low, pair)
            totals = jnp.sum(pair.astype(F32) * spread, axis=0, keepdims=True)
            for q in range(2):
                norm_ref[l + q : l + q + 1, :] = totals[:, q * members : (q + 1) * members]
        for store in stores:
            store.wait()

    return pl.pallas_call(
        body,
        out_shape=[
            jax.ShapeDtypeStruct((cells, members), BF16),
            jax.ShapeDtypeStruct((n_lam, members), F32),
        ],
        in_specs=[SMEM, SMEM] + [VMEM] * (n_obs + 1) + [ANY],
        out_specs=[ANY, VMEM],
        scratch_shapes=[
            pltpu.VMEM((members, width), F32),
            pltpu.VMEM((n_lam, members, width), F32),
            pltpu.VMEM((n_lam, members, members), BF16),
            pltpu.VMEM((n_lam, members, members), F32),
            pltpu.VMEM((n_lam, members, members), F32),
            pltpu.VMEM((count, chunk, members), BF16),
            pltpu.VMEM((count, chunk, members), BF16),
            pltpu.SemaphoreType.DMA((count,)),
            pltpu.SemaphoreType.DMA((count,)),
        ],
        compiler_params=params(52),
        cost_estimate=cost(2e9, 4 * cells * members),
        name="finish",
    )(place_obs, lambdas, *bands, field_gram, log_k)


def field_moments(log_k, total, first, chunk, count):
    members = log_k.shape[1]

    def body(x_ref, total_ref, out_ref, hold_ref, sem):
        copies = []
        for i in range(count):
            rows = pl.ds(first + i * chunk, chunk)
            copies.append(pltpu.make_async_copy(x_ref.at[rows], hold_ref.at[i], sem.at[i]))
            copies[i].start()
        eye = iota((members, members), 0) == iota((members, members), 1)
        centre = (jnp.where(eye, 1.0, 0.0) - 1.0 / members).astype(BF16)
        moments = total_ref[...]
        for i in range(count):
            copies[i].wait()
            anomalies = dot(hold_ref[i], centre).astype(BF16)
            moments = moments + dot(anomalies, anomalies, ((0,), (0,)))
        out_ref[...] = moments

    return pl.pallas_call(
        body,
        out_shape=jax.ShapeDtypeStruct((members, members), F32),
        in_specs=[ANY, VMEM],
        out_specs=VMEM,
        scratch_shapes=[
            pltpu.VMEM((count, chunk, members), BF16),
            pltpu.SemaphoreType.DMA((count,)),
        ],
        compiler_params=params(52),
        cost_estimate=cost(6.0e9, count * chunk * members * 2),
        name="field_moments",
    )(log_k, total)


def sum_band(gathered, after):
    n_tiles, band, width = gathered.shape

    def body(gathered_ref, after_ref, out_ref):
        total = gathered_ref[0].astype(F32)
        for t in range(1, n_tiles):
            total = total + gathered_ref[t].astype(F32)
        out_ref[...] = total

    return pl.pallas_call(
        body,
        out_shape=jax.ShapeDtypeStruct((band, width), F32),
        in_specs=[VMEM, VMEM],
        out_specs=VMEM,
        compiler_params=params(8),
        cost_estimate=cost(1e7, 1e6),
        name="sum_band",
    )(gathered, after)


def shifted(array, axis, step):
    n = lax.axis_size(axis)
    return lax.ppermute(array, axis, [(i, (i + step) % n) for i in range(n)])


def exchanged(arrays):
    moved = []
    for k, array in enumerate(arrays, 1):
        moved.append(shifted(array, "obs", k))
    return moved


def on_device(
    log_k, heads_pred, slot_well, tile_count, obs_values, obs_std, loc_blocks, taper, lambdas
):
    n_obs = lax.axis_size("obs")
    n_cell = lax.axis_size("cell")
    members = heads_pred.shape[1]
    place_obs = lax.axis_index("obs").astype(jnp.int32).reshape(1)
    sent, own_wells = send_rows(
        slot_well, tile_count, heads_pred, obs_values, obs_std, n_obs, n_cell
    )
    received = lax.all_to_all(sent, "cell", split_axis=0, concat_axis=0, tiled=True)
    wells = [own_wells] + [shifted(own_wells, "obs", k) for k in range(1, n_obs)]
    cells = log_k.shape[0]
    chunk = cells // 6
    moments = jnp.zeros((members, members), F32)
    moments = field_moments(log_k, moments, 0, chunk, 2)
    column_blocks = jnp.arange(n_obs, dtype=jnp.int32) * n_cell + lax.axis_index("cell")
    weights = jnp.sum(
        taper[:, :, None]
        * (loc_blocks[:, :, None] == column_blocks[None, None, :]).astype(F32),
        axis=1,
    )
    grams = block_grams(place_obs, received, wells, moments, n_obs)
    parts = [grams[0]] + exchanged(grams[1:])
    terms = tile_terms(weights, parts)
    gathered = lax.all_to_all(terms, "cell", split_axis=0, concat_axis=0, tiled=True)
    moments = field_moments(log_k, moments, 2 * chunk, chunk, 4)
    own_band = sum_band(gathered, moments)
    bands = [own_band] + exchanged([own_band] * (n_obs - 1))
    posterior, norms = finish(place_obs, lambdas, bands, moments, log_k, 6)
    return (posterior, norms[None])


def solution(mesh):
    return jax.shard_map(
        on_device,
        mesh=mesh,
        in_specs=(
            P(("obs", "cell"), None),
            P(("obs", "cell"), None),
            P(("obs", "cell")),
            P(("obs", "cell")),
            P(("obs", "cell"), None),
            P(("obs", "cell")),
            P(),
            P(),
            P(),
        ),
        out_specs=(P(("obs", "cell"), None), P(("obs", "cell"), None, None)),
        check_vma=False,
    )
```
